128 devices in a mesh: mem: 8 (over z, core), space: 16 (over x, y).
Axes of the slice: x: 4, y: 4, z: 4, core: 2. Of those that a mesh axis runs over, the one named last changes fastest.
Arguments:
- ensemble: float32 [128, 512, 16, 128], P(None, 'mem', 'space'), may hold values from -6 to 6
- obs_cells: int32 [128, 2048], P(('mem', 'space')), may hold values from 0 to 2047
- obs_values: float32 [128, 2048], P(('mem', 'space')), may hold values from -6 to 6
- obs_rinv: float32 [128, 2048], P(('mem', 'space')), may hold values from 0.2 to 5
- obs_count: int32 [128], P(('mem', 'space')), may hold values from 512 to 2048
Outputs:
- analysis: float32 [128, 512, 16, 128], P(None, 'mem', 'space')
The draws below stay inside these ranges and needn't reach their ends.
All inputs are finite; a program needn't handle non-finite values.
Results may differ from the reference program's by a relative error of at most 0.0003.
Values sent between devices are 32-bit elements; how exact they have to be, the bound alone decides.
No kernel may reach another device: no remote copies, remote signals or barrier semaphores. Data moves between devices by JAX's collectives and lax.ppermute only.
A program may use at most 128 MiB of HBM per device.

```python
import math
import jax
import jax.numpy as jnp
from jax import lax

MEMBERS = 512
BAND_LINES = 8
COLS_REG = 16
OBS_REG = 2048
NS_ITERS = 6
STEPS = 4
DOMAIN_PARTS = 128
ROWS = 128
CELLS_PER_REGION = 2048
N_MEM = 8
N_SPACE = 16


def set_ends(drawn, rng, smallest, top_value):
    shape = drawn.shape
    index_at = [jax.random.randint(jax.random.fold_in(rng, axis), (), 0, shape[axis]) for axis in range(len(shape))]
    drawn = drawn.at[tuple(index_at)].set(smallest)
    longest = shape.index(max(shape))
    index_at[longest] = (index_at[longest] + 1) % shape[longest]
    return drawn.at[tuple(index_at)].set(top_value)


def levels(rng, dims, pieces, low, high):
    def one(position, blocks):
        steps = jax.random.uniform(jax.random.fold_in(jax.random.fold_in(rng, 6), position), (blocks,), jnp.float32, low / len(pieces), high / len(pieces))
        return jnp.repeat(jnp.exp(steps), dims[position] // blocks).reshape((-1,) + (1,) * (len(dims) - position - 1))

    gain = one(*pieces[0])
    for cut in pieces[1:]:
        gain = gain * one(*cut)
    return gain


def normal_values(stream_key, shape, spread, reach, pieces=(), held_as=jnp.bfloat16):
    loudness = levels(stream_key, shape, pieces, -0.22, 0.18) if pieces else 1.0
    drawn = jax.random.normal(stream_key, shape, jnp.float32) * spread * loudness
    return jnp.minimum(jnp.maximum(drawn, -reach), reach).astype(held_as)


def setup_inputs(seed: int = 0) -> dict:
    key_of = jax.random.split(jax.random.key(seed), 6)
    ensemble = normal_values(key_of[0], (DOMAIN_PARTS, MEMBERS, N_SPACE, BAND_LINES * COLS_REG), 1.0, 6.0, ((1, 8), (2, 16)), jnp.float32)
    obs_cells = set_ends(jax.random.randint(key_of[1], (DOMAIN_PARTS, OBS_REG), 0, CELLS_PER_REGION), jax.random.fold_in(key_of[1], 1), 0, CELLS_PER_REGION - 1).astype(jnp.int32)
    obs_values = normal_values(key_of[2], (DOMAIN_PARTS, OBS_REG), 1.0, 6.0, ((0, 128),), jnp.float32)
    obs_rinv = jnp.clip(jnp.exp(math.log(5.0) - 3.218876 * jax.random.uniform(key_of[3], (DOMAIN_PARTS, OBS_REG), jnp.float32) ** levels(key_of[3], (DOMAIN_PARTS, OBS_REG), ((0, 128),), -0.2, 0.2)), 0.2, 5.0)
    obs_count = set_ends(jax.random.randint(key_of[4], (DOMAIN_PARTS,), OBS_REG // 4, OBS_REG + 1), jax.random.fold_in(key_of[4], 1), OBS_REG // 4, OBS_REG).astype(jnp.int32)
    return {"ensemble": ensemble, "obs_cells": obs_cells, "obs_values": obs_values, "obs_rinv": obs_rinv, "obs_count": obs_count}


DIFFUSION = 0.2
ADVECTION = 0.1

def eastward(center):
    following = jnp.roll(center, -1, axis=0)
    return jnp.concatenate([center[..., 1:], following[..., :1]], axis=-1)

def westward(center):
    previous = jnp.roll(center, 1, axis=0)
    return jnp.concatenate([previous[..., -1:], center[..., :-1]], axis=-1)

def advance(extended):
    center = extended[:, :, 1:-1]
    north = extended[:, :, :-2]
    south = extended[:, :, 2:]
    eastern = eastward(center)
    western = westward(center)
    return center + DIFFUSION * (north + south + eastern + western - 4.0 * center) - ADVECTION * center * (eastern - western + south - north)

def periodic(present_mesh_values):
    return advance(jnp.concatenate([present_mesh_values[:, :, -1:], present_mesh_values, present_mesh_values[:, :, :1]], axis=2))

def predicted_band(sample_band):
    for repeat in range(STEPS):
        sample_band = periodic(sample_band)
    return sample_band

def analyse(packed):
    members_now, cells, values, rinv, count = packed
    highest = lax.Precision.HIGHEST
    size = members_now.shape[0]
    mean_state = lax.optimization_barrier(jnp.mean(members_now, axis=0))
    anomaly = members_now - mean_state
    observed = jnp.take(members_now, cells, axis=1)
    obs_mean = lax.optimization_barrier(jnp.mean(observed, axis=0))
    active = (lax.iota(jnp.int32, cells.shape[0]) < count).astype(members_now.dtype)
    weight_root = jnp.sqrt(rinv * active / (size - 1.0))
    scaled = (observed - obs_mean) * weight_root
    observation_misfit = (values - obs_mean) * weight_root
    identity = jnp.eye(size, dtype=members_now.dtype)
    matrix = identity + jnp.dot(scaled, scaled.T, precision=highest)
    projected = jnp.dot(scaled, observation_misfit, precision=highest)
    frob_norm = jnp.sqrt(jnp.sum(matrix * matrix))
    iterate = matrix / frob_norm
    inverse_root = identity
    for repeat in range(NS_ITERS):
        update = 1.5 * identity - 0.5 * jnp.dot(inverse_root, iterate, precision=highest)
        iterate = jnp.dot(iterate, update, precision=highest)
        inverse_root = jnp.dot(update, inverse_root, precision=highest)
    inv_root = inverse_root / jnp.sqrt(frob_norm)
    inverted_matrix = jnp.dot(inv_root, inv_root, precision=highest)
    mean_shift = jnp.dot(inverted_matrix, projected, precision=highest)
    weights = inv_root + mean_shift[:, None]
    return mean_state + jnp.dot(weights.T, anomaly, precision=highest)

def reference(ensemble, obs_cells, obs_values, obs_rinv, obs_count):
    present_mesh_values = ensemble.reshape(DOMAIN_PARTS, N_MEM, MEMBERS // N_MEM, ROWS, COLS_REG)
    present_mesh_values = jnp.moveaxis(present_mesh_values, 1, 0)
    present_mesh_values = lax.map(predicted_band, present_mesh_values)
    present_mesh_values = jnp.moveaxis(present_mesh_values, 0, 1).reshape(DOMAIN_PARTS, MEMBERS, CELLS_PER_REGION)
    result = lax.map(analyse, (present_mesh_values, obs_cells, obs_values, obs_rinv, obs_count))
    return result.reshape(DOMAIN_PARTS, MEMBERS, N_SPACE, BAND_LINES * COLS_REG)
```

```python
import jax
import jax.numpy as jnp
from jax import lax
from jax.experimental import pallas as pl
from jax.experimental.pallas import tpu as pltpu
from jax.sharding import PartitionSpec as P

MEMBERS = 512
STEPS = 4
HALO = STEPS
LANES = 128
MESH = ("mem", "space")
RING = ("space", "mem")


NT = (((1,), (1,)), ((), ()))


def split(x):
    high = x.astype(jnp.bfloat16)
    return high, (x - high.astype(jnp.float32)).astype(jnp.bfloat16)


def dot(a, b, dims=(((1,), (0,)), ((), ()))):
    return lax.dot_general(a, b, dims, preferred_element_type=jnp.float32)


def dot3(a, b):
    return dot(a[0], b[0]) + (dot(a[0], b[1]) + dot(a[1], b[0]))


def obs_kernel(cells_ref, rinv_ref, values_ref, out_ref):
    cells = cells_ref[...]
    slots = cells.shape[1]
    strip = lax.broadcasted_iota(jnp.int32, (16, slots), 0) == (cells >> 7)
    lane = lax.broadcasted_iota(jnp.int32, (LANES, slots), 0) == (cells & 127)
    parts = []
    for value in (rinv_ref[...], rinv_ref[...] * values_ref[...]):
        for _ in range(3):
            part = value.astype(jnp.bfloat16).astype(jnp.float32)
            value = value - part
            parts.append(jnp.where(strip, part, 0.0).astype(jnp.bfloat16))
    total = dot(jnp.concatenate(parts, axis=0), lane.astype(jnp.float32).astype(jnp.bfloat16), NT)
    out_ref[0:16] = total[0:16] + total[16:32] + total[32:48]
    out_ref[16:32] = total[48:64] + total[64:80] + total[80:96]


def tiles_kernel(x_ref, u_ref, first_ref, last_ref):
    def strip(s, _):
        half = s // 8
        base = (s % 8) * 8
        for b in range(4):
            block = x_ref[pl.ds(s * 8 + 2 * b, 2)].reshape(LANES, LANES)
            turned = (block * 0.5).T
            for j in range(8):
                for g in range(2):
                    u_ref[base + j, pl.ds(64 * g + half * 4 + b, 8, stride=8), :] = turned[
                        j * 16 + 8 * g : j * 16 + 8 * g + 8
                    ]
        return 0

    lax.fori_loop(0, 16, strip, 0)

    def edge(r, _):
        first_ref[r] = u_ref[r, 0 : HALO * 8, :]
        last_ref[r] = u_ref[r, (16 - HALO) * 8 :, :]
        return 0

    lax.fori_loop(0, 64, edge, 0)


def sweep(load, store, columns, scale):
    width = len(columns)

    def row(r, n, c, s):
        west = load(r, columns[0] - 1)
        east = load(r, columns[-1] + 1)
        around = [west] + list(c) + [east]
        for i in range(width):
            p = around[i + 2] + s[i]
            q = around[i] + n[i]
            store(r, columns[i], scale * ((c[i] + (p + q)) - c[i] * (p - q)))

    def inner(r, carry):
        n, c = carry
        s = tuple(load(r + 1, k) for k in columns)
        row(r, n, c, s)
        return c, s

    n = tuple(pltpu.roll(load(63, k), 4, 0) for k in columns)
    c = tuple(load(0, k) for k in columns)
    wrapped = tuple(pltpu.roll(t, 4, 0) for t in c)
    n, c = lax.fori_loop(0, 63, inner, (n, c), unroll=3)
    row(63, n, c, wrapped)


def pieces(low, high, most):
    count = -(-(high - low) // most)
    edges = [low + (high - low) * i // count for i in range(count + 1)]
    return [list(range(a, b)) for a, b in zip(edges[:-1], edges[1:])]


def forecast(u_ref, west_ref, east_ref, a_ref, b_ref, f_ref):
    def at(col):
        return pl.ds(col * 8, 8)

    def start(r, col):
        if col < 0:
            return west_ref[r, at(col + HALO), :]
        if col >= 16:
            return east_ref[r, at(col - 16), :]
        return u_ref[r, at(col), :]

    def wide(ref):
        return lambda r, col: ref[r, at(col + HALO), :]

    def put(ref, shift):
        def store(r, col, value):
            ref[r, at(col + shift), :] = value

        return store

    loads = [start, wide(a_ref), wide(b_ref), wide(a_ref)]
    stores = [put(a_ref, HALO), put(b_ref, HALO), put(a_ref, HALO), put(f_ref, 0)]
    for step in range(STEPS):
        reach = HALO - 1 - step
        for columns in pieces(-reach, 16 + reach, 8):
            sweep(loads[step], stores[step], columns, 0.4 if step == STEPS - 1 else 0.2)


def analysis_kernel(
    u_ref, west_ref, east_ref, obs_ref, out_ref,
    a_ref, b_ref, f_ref, mean_ref, ah_ref, al_ref, bh_ref, bl_ref, proj_ref, t_ref, z_ref,
):
    forecast(u_ref, west_ref, east_ref, a_ref, b_ref, f_ref)
    proj_ref[...] = jnp.zeros_like(proj_ref)

    def strip(s, _):
        half = s // 8
        base = (s % 8) * 8
        blocks = []
        for b in range(4):
            rows = [
                f_ref[base + j, pl.ds(64 * g + half * 4 + b, 8, stride=8), :]
                for j in range(8)
                for g in range(2)
            ]
            blocks.append(jnp.concatenate(rows, axis=0).T)
        total = blocks[0] + blocks[1] + blocks[2] + blocks[3]
        mean = jnp.sum(total, axis=0, keepdims=True) * (1.0 / MEMBERS)
        mean_ref[pl.ds(s, 1)] = mean
        weight = obs_ref[pl.ds(s, 1)]
        root = jnp.sqrt(weight)
        misfit = obs_ref[pl.ds(s + 16, 1)] - weight * mean
        lanes = pl.ds(pl.multiple_of(s * LANES, LANES), LANES)
        for b in range(4):
            part = pl.ds(b * LANES, LANES)
            anomaly = blocks[b] - mean
            ah_ref[part, lanes], al_ref[part, lanes] = split(anomaly)
            bh_ref[part, lanes], bl_ref[part, lanes] = split(anomaly * root)
            proj_ref[part] += anomaly * misfit
        return 0

    lax.fori_loop(0, 16, strip, 0)

    shape = (MEMBERS, MEMBERS)
    diagonal = lax.broadcasted_iota(jnp.int32, shape, 0) == lax.broadcasted_iota(jnp.int32, shape, 1)

    def plus(coefficient, x):
        return x + jnp.where(diagonal, coefficient, 0.0)

    high, low = bh_ref[...], bl_ref[...]
    cross = dot(high, low, NT)
    matrix = plus(1.0, dot(high, high, NT) + (cross + dot(low, high, NT)))
    norm = jnp.sqrt(jnp.sum(jnp.sum(matrix * matrix, axis=0, keepdims=True), axis=1, keepdims=True))
    t_ref[...] = matrix * (1.0 / norm)

    for pair in range(3):
        t = t_ref[...]
        ts = split(t)
        square = dot3(ts, ts)
        inner = plus(1.6875, 0.0625 * square - 0.5625 * t)
        both = plus(2.25, dot3(split(square), split(inner)) - 2.4375 * t)
        us = split(both)
        if pair < 2:
            t_ref[...] = dot3(split(dot3(ts, us)), us)
        z_ref[...] = both if pair == 0 else dot3(us, split(z_ref[...]))

    root = z_ref[...] * (1.0 / jnp.sqrt(norm))
    projected = jnp.sum(proj_ref[...], axis=1, keepdims=True)
    once = jnp.sum(root * projected, axis=0, keepdims=True)
    once = jnp.broadcast_to(once, (8, MEMBERS)).T[:, 0:1]
    shift = jnp.sum(root * once, axis=0, keepdims=True)
    weights = split(root + shift)

    def columns(q, _):
        lanes = pl.ds(pl.multiple_of(q * 256, 256), 256)
        result = dot3(weights, (ah_ref[:, lanes], al_ref[:, lanes]))
        for i in range(2):
            piece = result[:, i * LANES : (i + 1) * LANES] + mean_ref[pl.ds(2 * q + i, 1)]
            out_ref[pl.ds((2 * q + i) * 8, 8)] = piece.reshape(8, 64, LANES)
        return 0

    lax.fori_loop(0, 8, columns, 0)


def vmem(count):
    return [pl.BlockSpec(memory_space=pltpu.VMEM) for _ in range(count)]


def f32(*shape):
    return jax.ShapeDtypeStruct(shape, jnp.float32)


def body(ensemble, obs_cells, obs_values, obs_rinv, obs_count):
    regions, block = ensemble.shape[0], ensemble.shape[1]
    params = pltpu.CompilerParams(vmem_limit_bytes=60 * 2**20)

    slots = lax.broadcasted_iota(jnp.int32, obs_cells.shape, 1)
    active = (slots < obs_count[:, None]).astype(jnp.float32)
    rinv = obs_rinv * active / (MEMBERS - 1.0)
    grids = pl.pallas_call(
        obs_kernel, out_shape=f32(32, LANES), in_specs=vmem(3), out_specs=vmem(1)[0],
        compiler_params=params, name="observations",
    )(obs_cells, rinv, obs_values)
    owner = [(r % 8) * 16 + r // 8 for r in range(regions)]
    grids = lax.ppermute(grids, MESH, list(enumerate(owner)))

    pieces_in = lax.all_to_all(
        ensemble.reshape(regions, block, LANES), RING, split_axis=0, concat_axis=0, tiled=True
    )
    tiles, first, last = pl.pallas_call(
        tiles_kernel,
        out_shape=[f32(64, 128, LANES), f32(64, HALO * 8, LANES), f32(64, HALO * 8, LANES)],
        in_specs=vmem(1), out_specs=vmem(3), compiler_params=params, name="tiles",
    )(pieces_in)
    after = [(owner[r], owner[(r + 1) % regions]) for r in range(regions)]
    before = [(owner[(r + 1) % regions], owner[r]) for r in range(regions)]
    west = lax.ppermute(last, MESH, after)
    east = lax.ppermute(first, MESH, before)
    half = pltpu.VMEM((MEMBERS, 2048), jnp.bfloat16)
    square = pltpu.VMEM((MEMBERS, MEMBERS), jnp.float32)
    wide = pltpu.VMEM((64, (16 + 2 * HALO) * 8, LANES), jnp.float32)
    analysed = pl.pallas_call(
        analysis_kernel,
        out_shape=f32(regions, block, LANES),
        in_specs=vmem(4), out_specs=vmem(1)[0],
        scratch_shapes=[
            wide, wide, pltpu.VMEM((64, 128, LANES), jnp.float32), pltpu.VMEM((16, LANES), jnp.float32),
            half, half, half, half, pltpu.VMEM((MEMBERS, LANES), jnp.float32), square, square,
        ],
        compiler_params=params, name="analysis",
    )(tiles, west, east, grids)
    returned = lax.all_to_all(analysed, RING, split_axis=0, concat_axis=0, tiled=True)
    return returned.reshape(ensemble.shape)


def solution(mesh):
    return jax.shard_map(
        body,
        mesh=mesh,
        in_specs=(
            P(None, "mem", "space", None),
            P(("mem", "space"), None),
            P(("mem", "space"), None),
            P(("mem", "space"), None),
            P(("mem", "space")),
        ),
        out_specs=P(None, "mem", "space", None),
        check_vma=False,
    )
```

```python
import jax
import jax.numpy as jnp
from jax import lax
from jax.experimental import pallas as pl
from jax.experimental.pallas import tpu as pltpu
from jax.sharding import PartitionSpec as P

MEMBERS = 512
STEPS = 4
HALO = STEPS
LANES = 128
MESH = ("mem", "space")
RING = ("space", "mem")


NT = (((1,), (1,)), ((), ()))


def split(x):
    high = x.astype(jnp.bfloat16)
    return high, (x - high.astype(jnp.float32)).astype(jnp.bfloat16)


def dot(a, b, dims=(((1,), (0,)), ((), ()))):
    return lax.dot_general(a, b, dims, preferred_element_type=jnp.float32)


def dot3(a, b):
    return dot(a[0], b[0]) + (dot(a[0], b[1]) + dot(a[1], b[0]))


def obs_kernel(cells_ref, rinv_ref, values_ref, out_ref):
    cells = cells_ref[...]
    slots = cells.shape[1]
    row, col = cells >> 4, cells & 15
    outer = ((col + 4) & 15) < 8
    place = (row >> 4) + jnp.where(outer, 8, 0)
    group = lax.broadcasted_iota(jnp.int32, (16, slots), 0) == place
    lane = lax.broadcasted_iota(jnp.int32, (LANES, slots), 0) == (row & 15) * 8 + (col & 7)
    parts = []
    for value in (rinv_ref[...], rinv_ref[...] * values_ref[...]):
        for _ in range(3):
            part = value.astype(jnp.bfloat16).astype(jnp.float32)
            value = value - part
            parts.append(jnp.where(group, part, 0.0).astype(jnp.bfloat16))
    total = dot(jnp.concatenate(parts, axis=0), lane.astype(jnp.float32).astype(jnp.bfloat16), NT)
    out_ref[0:16] = total[0:16] + total[16:32] + total[32:48]
    out_ref[16:32] = total[48:64] + total[64:80] + total[80:96]


def at(col):
    return pl.ds(col * 8, 8)


def tiles_kernel(x_ref, u_ref, first_ref, last_ref):
    def strip(s, _):
        half = s // 8
        base = (s % 8) * 8
        for b in range(4):
            block = x_ref[pl.ds(s * 8 + 2 * b, 2)].reshape(LANES, LANES)
            turned = (block * 0.5).T
            for j in range(8):
                for g in range(2):
                    u_ref[base + j, pl.ds(64 * g + half * 4 + b, 8, stride=8), :] = turned[
                        j * 16 + 8 * g : j * 16 + 8 * g + 8
                    ]
        return 0

    lax.fori_loop(0, 16, strip, 0)

    def edge(r, _):
        first_ref[r] = u_ref[r, 0 : HALO * 8, :]
        last_ref[r] = u_ref[r, (16 - HALO) * 8 :, :]
        return 0

    lax.fori_loop(0, 64, edge, 0, unroll=4)


def sweep(load, store, columns, scale):
    width = len(columns)

    def row(r, n, c, s):
        west = load(r, columns[0] - 1)
        east = load(r, columns[-1] + 1)
        around = [west] + list(c) + [east]
        for i in range(width):
            p = around[i + 2] + s[i]
            q = around[i] + n[i]
            store(r, columns[i], scale * ((c[i] + (p + q)) - c[i] * (p - q)))

    def body(r, carry):
        n, c = carry
        s = tuple(load(r + 1, k) for k in columns)
        row(r, n, c, s)
        return c, s

    n = tuple(pltpu.roll(load(63, k), 4, 0) for k in columns)
    c = tuple(load(0, k) for k in columns)
    wrapped = tuple(pltpu.roll(t, 4, 0) for t in c)
    n, c = lax.fori_loop(0, 63, body, (n, c), unroll=3)
    row(63, n, c, wrapped)


def pieces(low, high, most):
    count = -(-(high - low) // most)
    edges = [low + (high - low) * i // count for i in range(count + 1)]
    return [list(range(a, b)) for a, b in zip(edges[:-1], edges[1:])]


def scale_of(step):
    return 0.4 if step == STEPS - 1 else 0.2


def inner_kernel(u_ref, one_ref, two_ref, three_ref, inner_ref):
    levels = [u_ref, one_ref, two_ref, three_ref]
    for step in range(STEPS):
        low, high = step + 1, 15 - step

        def load(r, col, step=step):
            return levels[step][r, at(col - step), :]

        def store(r, col, value, step=step, low=low):
            if step < STEPS - 1:
                levels[step + 1][r, at(col - low), :] = value
            else:
                inner_ref[r, at(col & 7), :] = value

        for columns in pieces(low, high, 8):
            sweep(load, store, columns, scale_of(step))


def outer_forecast(levels, west_ref, east_ref, wests, easts, outer_ref):
    for step in range(STEPS):
        reach = HALO - step

        def load(r, col, step=step, reach=reach):
            if step == 0:
                if col < 0:
                    return west_ref[r, at(col + HALO), :]
                if col >= 16:
                    return east_ref[r, at(col - 16), :]
            elif col < step:
                return wests[step - 1][r, at(col + reach), :]
            elif col >= 16 - step:
                return easts[step - 1][r, at(col - 16 + step), :]
            return levels[step][r, at(col - step), :]

        def store(r, col, value, step=step, reach=reach):
            if step == STEPS - 1:
                outer_ref[r, at(col & 7), :] = value
            elif col < 8:
                wests[step][r, at(col + reach - 1), :] = value
            else:
                easts[step][r, at(col - 15 + step), :] = value

        sweep(load, store, list(range(1 - reach, step + 1)), scale_of(step))
        sweep(load, store, list(range(15 - step, 15 + reach)), scale_of(step))


def turned_rows(load, half, b, count):
    return jnp.concatenate([load(j, half * 4 + b) for j in range(count)], axis=0).T


def place_of(sub):
    return pl.ds(sub, 8, stride=8)


def gather_groups(part_ref, obs_ref, first_group, bh_ref, bl_ref, proj_ref):
    def group(q, _):
        half = q // 4
        base = (q % 4) * 16
        blocks = [
            turned_rows(lambda j, sub: part_ref[base + j, place_of(sub), :], half, b, 16)
            for b in range(4)
        ]
        total = blocks[0] + blocks[1] + blocks[2] + blocks[3]
        mean = jnp.sum(total, axis=0, keepdims=True) * (1.0 / MEMBERS)
        weight = obs_ref[pl.ds(first_group + q, 1)]
        root = jnp.sqrt(weight)
        misfit = obs_ref[pl.ds(first_group + q + 16, 1)] - weight * mean
        lanes = pl.ds(pl.multiple_of(q * LANES, LANES), LANES)
        for b in range(4):
            part = pl.ds(b * LANES, LANES)
            anomaly = blocks[b] - mean
            bh_ref[part, lanes], bl_ref[part, lanes] = split(anomaly * root)
            proj_ref[part] += anomaly * misfit
        return 0

    lax.fori_loop(0, 8, group, 0)
    high, low = bh_ref[...], bl_ref[...]
    return dot(high, high, NT) + (dot(high, low, NT) + dot(low, high, NT))


def inner_sums_kernel(inner_ref, obs_ref, matrix_ref, proj_ref, bh_ref, bl_ref):
    proj_ref[...] = jnp.zeros_like(proj_ref)
    matrix_ref[...] = gather_groups(inner_ref, obs_ref, 0, bh_ref, bl_ref, proj_ref)


def analysis_kernel(
    u_ref, one_ref, two_ref, three_ref, inner_ref, west_ref, east_ref, obs_ref, matrix_ref, sums_ref,
    out_ref,
    w1_ref, w2_ref, w3_ref, e1_ref, e2_ref, e3_ref, outer_ref,
    mean_ref, ah_ref, al_ref, bh_ref, bl_ref, proj_ref, t_ref, z_ref,
):
    outer_forecast(
        [u_ref, one_ref, two_ref, three_ref], west_ref, east_ref,
        [w1_ref, w2_ref, w3_ref], [e1_ref, e2_ref, e3_ref], outer_ref,
    )
    proj_ref[...] = sums_ref[...]
    matrix = matrix_ref[...] + gather_groups(outer_ref, obs_ref, 8, bh_ref, bl_ref, proj_ref)
    t_ref[...] = matrix

    low_half = lax.broadcasted_iota(jnp.int32, (8, LANES), 0) < 4

    def strip(s, _):
        half = s // 8
        base = (s % 8) * 8
        blocks = []
        for b in range(4):
            rows = []
            for j in range(8):
                sub = place_of(half * 4 + b)
                near = inner_ref[base + j, sub, :]
                far = outer_ref[base + j, sub, :]
                rows += [jnp.where(low_half, far, near), jnp.where(low_half, near, far)]
            blocks.append(jnp.concatenate(rows, axis=0).T)
        total = blocks[0] + blocks[1] + blocks[2] + blocks[3]
        mean = jnp.sum(total, axis=0, keepdims=True) * (1.0 / MEMBERS)
        mean_ref[pl.ds(s, 1)] = mean
        lanes = pl.ds(pl.multiple_of(s * LANES, LANES), LANES)
        for b in range(4):
            part = pl.ds(b * LANES, LANES)
            ah_ref[part, lanes], al_ref[part, lanes] = split(blocks[b] - mean)
        return 0

    lax.fori_loop(0, 16, strip, 0)

    shape = (MEMBERS, MEMBERS)
    diagonal = lax.broadcasted_iota(jnp.int32, shape, 0) == lax.broadcasted_iota(jnp.int32, shape, 1)

    def plus(coefficient, x):
        return x + jnp.where(diagonal, coefficient, 0.0)

    matrix = plus(1.0, t_ref[...])
    norm = jnp.sqrt(jnp.sum(jnp.sum(matrix * matrix, axis=0, keepdims=True), axis=1, keepdims=True))
    t_ref[...] = matrix * (1.0 / norm)

    for pair in range(3):
        t = t_ref[...]
        ts = split(t)
        square = dot3(ts, ts)
        inner = plus(1.6875, 0.0625 * square - 0.5625 * t)
        both = plus(2.25, dot3(split(square), split(inner)) - 2.4375 * t)
        us = split(both)
        if pair < 2:
            t_ref[...] = dot3(split(dot3(ts, us)), us)
        z_ref[...] = both if pair == 0 else dot3(us, split(z_ref[...]))

    root = z_ref[...] * (1.0 / jnp.sqrt(norm))
    projected = jnp.sum(proj_ref[...], axis=1, keepdims=True)
    once = jnp.sum(root * projected, axis=0, keepdims=True)
    once = jnp.broadcast_to(once, (8, MEMBERS)).T[:, 0:1]
    shift = jnp.sum(root * once, axis=0, keepdims=True)
    weights = split(root + shift)

    def result_of(q, _):
        lanes = pl.ds(pl.multiple_of(q * 256, 256), 256)
        result = dot3(weights, (ah_ref[:, lanes], al_ref[:, lanes]))
        for i in range(2):
            piece = result[:, i * LANES : (i + 1) * LANES] + mean_ref[pl.ds(2 * q + i, 1)]
            out_ref[pl.ds((2 * q + i) * 8, 8)] = piece.reshape(8, 64, LANES)
        return 0

    lax.fori_loop(0, 8, result_of, 0)


def vmem(count):
    return [pl.BlockSpec(memory_space=pltpu.VMEM) for _ in range(count)]


def call(kernel, outs, scratch, limit, flops, name, *operands):
    operands = [pltpu.with_memory_space_constraint(x, pltpu.VMEM) for x in operands]
    return pl.pallas_call(
        kernel,
        out_shape=[pltpu.VMEM(shape, jnp.float32) for shape in outs],
        in_specs=vmem(len(operands)),
        out_specs=vmem(len(outs)),
        scratch_shapes=[pltpu.VMEM(*shape) for shape in scratch],
        compiler_params=pltpu.CompilerParams(vmem_limit_bytes=limit * 2**20),
        cost_estimate=pl.CostEstimate(flops=flops, transcendentals=0, bytes_accessed=2**20),
        name=name,
    )(*operands)


def columns(count):
    return (64, count * 8, LANES)


def body(ensemble, obs_cells, obs_values, obs_rinv, obs_count):
    regions, block = ensemble.shape[0], ensemble.shape[1]
    owner = [(r % 8) * 16 + r // 8 for r in range(regions)]
    after = [(owner[r], owner[(r + 1) % regions]) for r in range(regions)]
    before = [(owner[(r + 1) % regions], owner[r]) for r in range(regions)]
    unit = 10**9

    slots = lax.broadcasted_iota(jnp.int32, obs_cells.shape, 1)
    active = (slots < obs_count[:, None]).astype(jnp.float32)
    rinv = obs_rinv * active / (MEMBERS - 1.0)
    grids = pl.pallas_call(
        obs_kernel, out_shape=pltpu.VMEM((32, LANES), jnp.float32), in_specs=vmem(3), out_specs=vmem(1)[0],
        compiler_params=pltpu.CompilerParams(vmem_limit_bytes=4 * 2**20), name="observations",
    )(obs_cells, rinv, obs_values)
    grids = lax.ppermute(grids, MESH, list(enumerate(owner)))
    pieces_in = lax.all_to_all(
        ensemble.reshape(regions, block, LANES), RING, split_axis=0, concat_axis=0, tiled=True
    )
    pieces_in, grids = lax.optimization_barrier((pieces_in, grids))
    tiles, first, last = call(
        tiles_kernel, [columns(16), columns(HALO), columns(HALO)], [], 8, unit, "tiles", pieces_in
    )
    west = lax.ppermute(last, MESH, after)
    east = lax.ppermute(first, MESH, before)
    levels = call(
        inner_kernel, [columns(14), columns(12), columns(10), columns(8)], [], 2, 4 * unit, "inner", tiles
    )

    f32, bf16 = jnp.float32, jnp.bfloat16
    half = ((MEMBERS, 1024), bf16)
    whole = ((MEMBERS, 2048), bf16)
    square = ((MEMBERS, MEMBERS), f32)
    sums = (MEMBERS, LANES)
    matrix, projected = call(
        inner_sums_kernel, [square[0], sums], [half, half], 8, 6 * unit, "inner_sums", levels[3], grids
    )
    side = (columns(HALO), f32)
    (analysed,) = call(
        analysis_kernel,
        [(regions, block, LANES)],
        [side] * 6
        + [(columns(8), f32), ((16, LANES), f32), whole, whole, half, half, (sums, f32), square, square],
        24, 30 * unit, "analysis", tiles, *levels, west, east, grids, matrix, projected,
    )
    returned = lax.all_to_all(analysed, RING, split_axis=0, concat_axis=0, tiled=True)
    return returned.reshape(ensemble.shape)


def solution(mesh):
    return jax.shard_map(
        body,
        mesh=mesh,
        in_specs=(
            P(None, "mem", "space", None),
            P(("mem", "space"), None),
            P(("mem", "space"), None),
            P(("mem", "space"), None),
            P(("mem", "space")),
        ),
        out_specs=P(None, "mem", "space", None),
        check_vma=False,
    )
```

```python
import jax
import jax.numpy as jnp
from jax import lax
from jax.experimental import pallas as pl
from jax.experimental.pallas import tpu as pltpu
from jax.sharding import PartitionSpec as P

MEMBERS = 512
STEPS = 4
HALO = STEPS
LANES = 128
MESH = ("mem", "space")
RING = ("space", "mem")


NT = (((1,), (1,)), ((), ()))


def split(x):
    high = x.astype(jnp.bfloat16)
    return high, (x - high.astype(jnp.float32)).astype(jnp.bfloat16)


def dot(a, b, dims=(((1,), (0,)), ((), ()))):
    return lax.dot_general(a, b, dims, preferred_element_type=jnp.float32)


def dot3(a, b):
    return dot(a[0], b[0]) + (dot(a[0], b[1]) + dot(a[1], b[0]))


def obs_kernel(cells_ref, rinv_ref, values_ref, out_ref):
    cells = cells_ref[...]
    slots = cells.shape[1]
    row, col = cells >> 4, cells & 15
    outer = ((col + 4) & 15) < 8
    place = (row >> 4) + jnp.where(outer, 8, 0)
    group = lax.broadcasted_iota(jnp.int32, (16, slots), 0) == place
    lane = lax.broadcasted_iota(jnp.int32, (LANES, slots), 0) == ((row & 7) * 2 + ((row >> 3) & 1)) * 8 + (col & 7)
    parts = []
    for value in (rinv_ref[...], rinv_ref[...] * values_ref[...]):
        for _ in range(3):
            part = value.astype(jnp.bfloat16).astype(jnp.float32)
            value = value - part
            parts.append(jnp.where(group, part, 0.0).astype(jnp.bfloat16))
    total = dot(jnp.concatenate(parts, axis=0), lane.astype(jnp.float32).astype(jnp.bfloat16), NT)
    out_ref[0:16] = total[0:16] + total[16:32] + total[32:48]
    out_ref[16:32] = total[48:64] + total[64:80] + total[80:96]


def at(col):
    return pl.ds(col * 8, 8)


def tiles_kernel(x_ref, u_ref, first_ref, last_ref, block_ref, sems):
    def arrival(s):
        part = pl.ds(s * 8, 8)
        return pltpu.make_async_copy(x_ref.at[part], block_ref.at[part], sems.at[s])

    for s in range(16):
        arrival(s).start()

    def strip(s, _):
        half = s // 8
        base = (s % 8) * 8
        arrival(s).wait()
        for b in range(4):
            block = block_ref[pl.ds(s * 8 + 2 * b, 2)].reshape(LANES, LANES)
            turned = (block * 0.5).T
            for j in range(8):
                for g in range(2):
                    u_ref[base + j, pl.ds(64 * g + half * 4 + b, 8, stride=8), :] = turned[
                        j * 16 + 8 * g : j * 16 + 8 * g + 8
                    ]
        return 0

    lax.fori_loop(0, 16, strip, 0)

    def edge(r, _):
        first_ref[r] = u_ref[r, 0 : HALO * 8, :]
        last_ref[r] = u_ref[r, (16 - HALO) * 8 :, :]
        return 0

    lax.fori_loop(0, 64, edge, 0, unroll=4)


def sweep(load, store, columns, scale):
    width = len(columns)

    def row(r, n, c, s):
        west = load(r, columns[0] - 1)
        east = load(r, columns[-1] + 1)
        around = [west] + list(c) + [east]
        for i in range(width):
            p = around[i + 2] + s[i]
            q = around[i] + n[i]
            store(r, columns[i], scale * ((c[i] + (p + q)) - c[i] * (p - q)))

    def body(r, carry):
        n, c = carry
        s = tuple(load(r + 1, k) for k in columns)
        row(r, n, c, s)
        return c, s

    n = tuple(pltpu.roll(load(63, k), 4, 0) for k in columns)
    c = tuple(load(0, k) for k in columns)
    wrapped = tuple(pltpu.roll(t, 4, 0) for t in c)
    n, c = lax.fori_loop(0, 63, body, (n, c), unroll=3)
    row(63, n, c, wrapped)


def pieces(low, high, most):
    count = -(-(high - low) // most)
    edges = [low + (high - low) * i // count for i in range(count + 1)]
    return [list(range(a, b)) for a, b in zip(edges[:-1], edges[1:])]


def scale_of(step):
    return 0.4 if step == STEPS - 1 else 0.2


def inner_kernel(u_ref, one_ref, two_ref, three_ref, inner_ref):
    levels = [u_ref, one_ref, two_ref, three_ref]
    for step in range(STEPS):
        low, high = step + 1, 15 - step

        def load(r, col, step=step):
            return levels[step][r, at(col - step), :]

        def store(r, col, value, step=step, low=low):
            if step < STEPS - 1:
                levels[step + 1][r, at(col - low), :] = value
            else:
                inner_ref[r, at(col & 7), :] = value

        for columns in pieces(low, high, 8):
            sweep(load, store, columns, scale_of(step))


def outer_forecast(levels, west_ref, east_ref, wests, easts, outer_ref):
    for step in range(STEPS):
        reach = HALO - step

        def load(r, col, step=step, reach=reach):
            if step == 0:
                if col < 0:
                    return west_ref[r, at(col + HALO), :]
                if col >= 16:
                    return east_ref[r, at(col - 16), :]
            elif col < step:
                return wests[step - 1][r, at(col + reach), :]
            elif col >= 16 - step:
                return easts[step - 1][r, at(col - 16 + step), :]
            return levels[step][r, at(col - step), :]

        def store(r, col, value, step=step, reach=reach):
            if step == STEPS - 1:
                outer_ref[r, at(col & 7), :] = value
            elif col < 8:
                wests[step][r, at(col + reach - 1), :] = value
            else:
                easts[step][r, at(col - 15 + step), :] = value

        sweep(load, store, list(range(1 - reach, step + 1)), scale_of(step))
        sweep(load, store, list(range(15 - step, 15 + reach)), scale_of(step))


def gather_groups(part_ref, obs_ref, first_group, mean_ref, ah_ref, al_ref, bh_ref, bl_ref, proj_ref):
    def group(q, _):
        half = q // 4
        base = (q % 4) * 16
        blocks = []
        for b in range(4):
            place = pl.ds(half * 4 + b, 8, stride=8)
            rows = [part_ref[base + 8 * p + j, place, :] for j in range(8) for p in range(2)]
            blocks.append(jnp.concatenate(rows, axis=0).T)
        total = blocks[0] + blocks[1] + blocks[2] + blocks[3]
        mean = jnp.sum(total, axis=0, keepdims=True) * (1.0 / MEMBERS)
        mean_ref[pl.ds(q, 1)] = mean
        weight = obs_ref[pl.ds(first_group + q, 1)]
        root = jnp.sqrt(weight)
        misfit = obs_ref[pl.ds(first_group + q + 16, 1)] - weight * mean
        lanes = pl.ds(pl.multiple_of(q * LANES, LANES), LANES)
        for b in range(4):
            part = pl.ds(b * LANES, LANES)
            anomaly = blocks[b] - mean
            ah_ref[part, lanes], al_ref[part, lanes] = split(anomaly)
            bh_ref[part, lanes], bl_ref[part, lanes] = split(anomaly * root)
            proj_ref[part] += anomaly * misfit
        return 0

    lax.fori_loop(0, 8, group, 0)
    high, low = bh_ref[...], bl_ref[...]
    return dot(high, high, NT) + (dot(high, low, NT) + dot(low, high, NT))


def inner_sums_kernel(inner_ref, obs_ref, matrix_ref, proj_ref, mean_ref, ah_ref, al_ref, bh_ref, bl_ref):
    proj_ref[...] = jnp.zeros_like(proj_ref)
    matrix_ref[...] = gather_groups(
        inner_ref, obs_ref, 0, mean_ref, ah_ref, al_ref, bh_ref, bl_ref, proj_ref
    )


def analysis_kernel(
    u_ref, one_ref, two_ref, three_ref, west_ref, east_ref, obs_ref,
    matrix_ref, sums_ref, mean_in_ref, ah_in_ref, al_in_ref,
    out_ref,
    w1_ref, w2_ref, w3_ref, e1_ref, e2_ref, e3_ref, outer_ref,
    mean_ref, ah_ref, al_ref, bh_ref, bl_ref, proj_ref, y_ref, z_ref,
):
    outer_forecast(
        [u_ref, one_ref, two_ref, three_ref], west_ref, east_ref,
        [w1_ref, w2_ref, w3_ref], [e1_ref, e2_ref, e3_ref], outer_ref,
    )
    proj_ref[...] = sums_ref[...]
    matrix = matrix_ref[...] + gather_groups(
        outer_ref, obs_ref, 8, mean_ref, ah_ref, al_ref, bh_ref, bl_ref, proj_ref
    )

    shape = (MEMBERS, MEMBERS)
    diagonal = lax.broadcasted_iota(jnp.int32, shape, 0) == lax.broadcasted_iota(jnp.int32, shape, 1)

    def plus(coefficient, x):
        return x + jnp.where(diagonal, coefficient, 0.0)

    matrix = plus(1.0, matrix)
    norm = jnp.sqrt(jnp.sum(jnp.sum(matrix * matrix, axis=0, keepdims=True), axis=1, keepdims=True))
    y_ref[...] = matrix * (1.0 / norm)

    identity = 1.0
    for pair in range(3):
        y = y_ref[...]
        t = y
        if pair:
            t = identity * y + dot3(split(z_ref[...]), split(y))
        ts = split(t)
        square = dot3(ts, ts)
        extra = 1.6875 * square - 2.4375 * t + dot3(split(square), split(0.0625 * square - 0.5625 * t))
        es = split(extra)
        if pair < 2:
            y_ref[...] = 2.25 * y + dot3(split(y), es)
        if pair:
            z = z_ref[...]
            extra = 2.25 * z + identity * extra + dot3(es, split(z))
        z_ref[...] = extra
        identity = 2.25 * identity

    root = plus(identity, z_ref[...]) * (1.0 / jnp.sqrt(norm))
    projected = jnp.sum(proj_ref[...], axis=1, keepdims=True)
    once = jnp.sum(root * projected, axis=0, keepdims=True)
    once = jnp.broadcast_to(once, (8, MEMBERS)).T[:, 0:1]
    shift = jnp.sum(root * once, axis=0, keepdims=True)
    weights = split(root + shift)

    lane = lax.broadcasted_iota(jnp.int32, (MEMBERS, LANES), 1)
    low = (lane & 7) < 4
    even = (lane & 8) == 0

    def result_of(q, _):
        lanes = pl.ds(pl.multiple_of(q * LANES, LANES), LANES)
        cells = [
            jnp.concatenate([near[:, lanes], far[:, lanes]], axis=1)
            for near, far in ((ah_in_ref, ah_ref), (al_in_ref, al_ref))
        ]
        result = dot3(weights, cells)
        near = result[:, :LANES] + mean_in_ref[pl.ds(q, 1)]
        far = result[:, LANES:] + mean_ref[pl.ds(q, 1)]
        left = jnp.where(low, far, near)
        right = jnp.where(low, near, far)
        upper = jnp.where(even, left, pltpu.roll(right, 8, 1))
        lower = jnp.where(even, pltpu.roll(left, LANES - 8, 1), right)
        out_ref[pl.ds(q * 16, 8)] = upper.reshape(8, 64, LANES)
        out_ref[pl.ds(q * 16 + 8, 8)] = lower.reshape(8, 64, LANES)
        return 0

    lax.fori_loop(0, 8, result_of, 0)


def vmem(count):
    return [pl.BlockSpec(memory_space=pltpu.VMEM) for _ in range(count)]


def in_vmem(x):
    return pltpu.with_memory_space_constraint(x, pltpu.VMEM)


def call(kernel, outs, scratch, limit, flops, name, *operands, specs=None):
    return pl.pallas_call(
        kernel,
        out_shape=[pltpu.VMEM(*out) for out in outs],
        in_specs=specs or vmem(len(operands)),
        out_specs=vmem(len(outs)),
        scratch_shapes=scratch,
        compiler_params=pltpu.CompilerParams(vmem_limit_bytes=limit * 2**20),
        cost_estimate=pl.CostEstimate(flops=flops, transcendentals=0, bytes_accessed=2**20),
        name=name,
    )(*operands)


def columns(count):
    return (64, count * 8, LANES), jnp.float32


def body(ensemble, obs_cells, obs_values, obs_rinv, obs_count):
    regions, block = ensemble.shape[0], ensemble.shape[1]
    owner = [(r % 8) * 16 + r // 8 for r in range(regions)]
    after = [(owner[r], owner[(r + 1) % regions]) for r in range(regions)]
    before = [(owner[(r + 1) % regions], owner[r]) for r in range(regions)]
    unit = 10**9

    slots = lax.broadcasted_iota(jnp.int32, obs_cells.shape, 1)
    active = (slots < obs_count[:, None]).astype(jnp.float32)
    rinv = obs_rinv * active / (MEMBERS - 1.0)
    grids = pl.pallas_call(
        obs_kernel, out_shape=pltpu.VMEM((32, LANES), jnp.float32), in_specs=vmem(3), out_specs=vmem(1)[0],
        compiler_params=pltpu.CompilerParams(vmem_limit_bytes=4 * 2**20), name="observations",
    )(obs_cells, rinv, obs_values)
    grids = lax.ppermute(grids, MESH, list(enumerate(owner)))
    pieces_in = lax.all_to_all(
        ensemble.reshape(regions, block, LANES), RING, split_axis=0, concat_axis=0, tiled=True
    )
    pieces_in, grids = lax.optimization_barrier((pieces_in, grids))
    f32, bf16 = jnp.float32, jnp.bfloat16
    tiles, first, last = call(
        tiles_kernel, [columns(16), columns(HALO), columns(HALO)],
        [pltpu.VMEM((regions, block, LANES), f32), pltpu.SemaphoreType.DMA((16,))],
        8, unit, "tiles", pieces_in, specs=[pl.BlockSpec(memory_space=pl.ANY)],
    )
    west = lax.ppermute(last, MESH, after)
    east = lax.ppermute(first, MESH, before)
    *levels, inner = call(
        inner_kernel, [columns(14), columns(12), columns(10), columns(8)], [], 2, 4 * unit, "inner",
        in_vmem(tiles),
    )
    half = (MEMBERS, 1024), bf16
    square = (MEMBERS, MEMBERS), f32
    sums = (MEMBERS, LANES), f32
    means = (8, LANES), f32
    partial = call(
        inner_sums_kernel, [square, sums, means, half, half], [pltpu.VMEM(*half)] * 2,
        8, 6 * unit, "inner_sums", in_vmem(inner), in_vmem(grids),
    )
    inputs = [tiles, *levels, west, east, grids, *partial]
    (analysed,) = call(
        analysis_kernel,
        [((regions, block, LANES), f32)],
        [
            pltpu.VMEM(*shape)
            for shape in [columns(HALO)] * 6 + [columns(8), means] + [half] * 4 + [sums, square, square]
        ],
        24, 30 * unit, "analysis", *[in_vmem(x) for x in inputs],
    )
    returned = lax.all_to_all(analysed, RING, split_axis=0, concat_axis=0, tiled=True)
    return returned.reshape(ensemble.shape)


def solution(mesh):
    return jax.shard_map(
        body,
        mesh=mesh,
        in_specs=(
            P(None, "mem", "space", None),
            P(("mem", "space"), None),
            P(("mem", "space"), None),
            P(("mem", "space"), None),
            P(("mem", "space")),
        ),
        out_specs=P(None, "mem", "space", None),
        check_vma=False,
    )
```

```python
import jax
import jax.numpy as jnp
from jax import lax
from jax.experimental import pallas as pl
from jax.experimental.pallas import tpu as pltpu
from jax.sharding import PartitionSpec as P

MEMBERS = 512
STEPS = 4
HALO = STEPS
LANES = 128
MESH = ("mem", "space")

def column_strip(place):
    return (place & 12) + ((place - (place >> 2)) & 3)


def strip_column(strip):
    return (strip & 12) + ((strip + (strip >> 2)) & 3)


OWNER = [
    (2 * ((k - place) & 3) + core) * 16 + column_strip(place)
    for place in range(16)
    for k in range(4)
    for core in range(2)
]


NT = (((1,), (1,)), ((), ()))


def split(x):
    high = x.astype(jnp.bfloat16)
    return high, (x - high.astype(jnp.float32)).astype(jnp.bfloat16)


def dot(a, b, dims=(((1,), (0,)), ((), ()))):
    return lax.dot_general(a, b, dims, preferred_element_type=jnp.float32)


def dot3(a, b):
    return dot(a[0], b[0]) + (dot(a[0], b[1]) + dot(a[1], b[0]))


def obs_kernel(cells_ref, rinv_ref, values_ref, out_ref):
    cells = cells_ref[...]
    slots = cells.shape[1]
    row, col = cells >> 4, cells & 15
    outer = ((col + 4) & 15) < 8
    place = (row >> 4) + jnp.where(outer, 8, 0)
    group = lax.broadcasted_iota(jnp.int32, (16, slots), 0) == place
    lane = lax.broadcasted_iota(jnp.int32, (LANES, slots), 0) == ((row & 7) * 2 + ((row >> 3) & 1)) * 8 + (col & 7)
    parts = []
    for value in (rinv_ref[...], rinv_ref[...] * values_ref[...]):
        for _ in range(3):
            part = value.astype(jnp.bfloat16).astype(jnp.float32)
            value = value - part
            parts.append(jnp.where(group, part, 0.0).astype(jnp.bfloat16))
    total = dot(jnp.concatenate(parts, axis=0), lane.astype(jnp.float32).astype(jnp.bfloat16), NT)
    out_ref[0:16] = total[0:16] + total[16:32] + total[32:48]
    out_ref[16:32] = total[48:64] + total[64:80] + total[80:96]


def at(col):
    return pl.ds(col * 8, 8)


def tiles_kernel(x_ref, u_ref, first_ref, last_ref, block_ref, sems):
    def arrival(s):
        part = pl.ds(s * 8, 8)
        return pltpu.make_async_copy(x_ref.at[part], block_ref.at[part], sems.at[s])

    for s in range(16):
        arrival(s).start()

    def column(place, _):
        s = column_strip(place)
        half = s // 8
        base = (s % 8) * 8
        arrival(place).wait()
        for b in range(4):
            block = block_ref[pl.ds(place * 8 + ((b + place) & 3) * 2, 2)].reshape(LANES, LANES)
            turned = (block * 0.5).T
            for j in range(8):
                for g in range(2):
                    u_ref[base + j, pl.ds(64 * g + half * 4 + b, 8, stride=8), :] = turned[
                        j * 16 + 8 * g : j * 16 + 8 * g + 8
                    ]
        return 0

    lax.fori_loop(0, 16, column, 0)

    def edge(r, _):
        first_ref[r] = u_ref[r, 0 : HALO * 8, :]
        last_ref[r] = u_ref[r, (16 - HALO) * 8 :, :]
        return 0

    lax.fori_loop(0, 64, edge, 0, unroll=4)


def sweep(load, store, columns, scale):
    width = len(columns)

    def row(r, n, c, s):
        west = load(r, columns[0] - 1)
        east = load(r, columns[-1] + 1)
        around = [west] + list(c) + [east]
        for i in range(width):
            p = around[i + 2] + s[i]
            q = around[i] + n[i]
            store(r, columns[i], scale * ((c[i] + (p + q)) - c[i] * (p - q)))

    def body(r, carry):
        n, c = carry
        s = tuple(load(r + 1, k) for k in columns)
        row(r, n, c, s)
        return c, s

    n = tuple(pltpu.roll(load(63, k), 4, 0) for k in columns)
    c = tuple(load(0, k) for k in columns)
    wrapped = tuple(pltpu.roll(t, 4, 0) for t in c)
    n, c = lax.fori_loop(0, 63, body, (n, c), unroll=3)
    row(63, n, c, wrapped)


def pieces(low, high, most):
    count = -(-(high - low) // most)
    edges = [low + (high - low) * i // count for i in range(count + 1)]
    return [list(range(a, b)) for a, b in zip(edges[:-1], edges[1:])]


def scale_of(step):
    return 0.4 if step == STEPS - 1 else 0.2


def inner_kernel(u_ref, one_ref, two_ref, three_ref, inner_ref):
    levels = [u_ref, one_ref, two_ref, three_ref]
    for step in range(STEPS):
        low, high = step + 1, 15 - step

        def load(r, col, step=step):
            return levels[step][r, at(col - step), :]

        def store(r, col, value, step=step, low=low):
            if step < STEPS - 1:
                levels[step + 1][r, at(col - low), :] = value
            else:
                inner_ref[r, at(col & 7), :] = value

        for columns in pieces(low, high, 8):
            sweep(load, store, columns, scale_of(step))


def outer_forecast(levels, west_ref, east_ref, wests, easts, outer_ref):
    for step in range(STEPS):
        reach = HALO - step

        def load(r, col, step=step, reach=reach):
            if step == 0:
                if col < 0:
                    return west_ref[r, at(col + HALO), :]
                if col >= 16:
                    return east_ref[r, at(col - 16), :]
            elif col < step:
                return wests[step - 1][r, at(col + reach), :]
            elif col >= 16 - step:
                return easts[step - 1][r, at(col - 16 + step), :]
            return levels[step][r, at(col - step), :]

        def store(r, col, value, step=step, reach=reach):
            if step == STEPS - 1:
                outer_ref[r, at(col & 7), :] = value
            elif col < 8:
                wests[step][r, at(col + reach - 1), :] = value
            else:
                easts[step][r, at(col - 15 + step), :] = value

        sweep(load, store, list(range(1 - reach, step + 1)), scale_of(step))
        sweep(load, store, list(range(15 - step, 15 + reach)), scale_of(step))


def gather_groups(part_ref, obs_ref, first_group, mean_ref, ah_ref, al_ref, bh_ref, bl_ref, proj_ref):
    def group(q, _):
        half = q // 4
        base = (q % 4) * 16
        blocks = []
        for b in range(4):
            place = pl.ds(half * 4 + b, 8, stride=8)
            rows = [part_ref[base + 8 * p + j, place, :] for j in range(8) for p in range(2)]
            blocks.append(jnp.concatenate(rows, axis=0).T)
        total = blocks[0] + blocks[1] + blocks[2] + blocks[3]
        mean = jnp.sum(total, axis=0, keepdims=True) * (1.0 / MEMBERS)
        mean_ref[pl.ds(q, 1)] = mean
        weight = obs_ref[pl.ds(first_group + q, 1)]
        root = jnp.sqrt(weight)
        misfit = obs_ref[pl.ds(first_group + q + 16, 1)] - weight * mean
        lanes = pl.ds(pl.multiple_of(q * LANES, LANES), LANES)
        for b in range(4):
            part = pl.ds(b * LANES, LANES)
            anomaly = blocks[b] - mean
            ah_ref[part, lanes], al_ref[part, lanes] = split(anomaly)
            bh_ref[part, lanes], bl_ref[part, lanes] = split(anomaly * root)
            proj_ref[part] += anomaly * misfit
        return 0

    lax.fori_loop(0, 8, group, 0)
    high, low = bh_ref[...], bl_ref[...]
    return dot(high, high, NT) + (dot(high, low, NT) + dot(low, high, NT))


def inner_sums_kernel(inner_ref, obs_ref, matrix_ref, proj_ref, mean_ref, ah_ref, al_ref, bh_ref, bl_ref):
    proj_ref[...] = jnp.zeros_like(proj_ref)
    matrix_ref[...] = gather_groups(
        inner_ref, obs_ref, 0, mean_ref, ah_ref, al_ref, bh_ref, bl_ref, proj_ref
    )


def analysis_kernel(
    u_ref, one_ref, two_ref, three_ref, west_ref, east_ref, obs_ref,
    matrix_ref, sums_ref, mean_in_ref, ah_in_ref, al_in_ref,
    out_ref,
    w1_ref, w2_ref, w3_ref, e1_ref, e2_ref, e3_ref, outer_ref,
    mean_ref, ah_ref, al_ref, bh_ref, bl_ref, proj_ref, y_ref, z_ref,
):
    outer_forecast(
        [u_ref, one_ref, two_ref, three_ref], west_ref, east_ref,
        [w1_ref, w2_ref, w3_ref], [e1_ref, e2_ref, e3_ref], outer_ref,
    )
    proj_ref[...] = sums_ref[...]
    matrix = matrix_ref[...] + gather_groups(
        outer_ref, obs_ref, 8, mean_ref, ah_ref, al_ref, bh_ref, bl_ref, proj_ref
    )

    shape = (MEMBERS, MEMBERS)
    diagonal = lax.broadcasted_iota(jnp.int32, shape, 0) == lax.broadcasted_iota(jnp.int32, shape, 1)

    def plus(coefficient, x):
        return x + jnp.where(diagonal, coefficient, 0.0)

    matrix = plus(1.0, matrix)
    norm = jnp.sqrt(jnp.sum(jnp.sum(matrix * matrix, axis=0, keepdims=True), axis=1, keepdims=True))
    y_ref[...] = matrix * (1.0 / norm)

    identity = 1.0
    for pair in range(3):
        y = y_ref[...]
        t = y
        if pair:
            t = identity * y + dot3(split(z_ref[...]), split(y))
        ts = split(t)
        square = dot3(ts, ts)
        extra = 1.6875 * square - 2.4375 * t + dot3(split(square), split(0.0625 * square - 0.5625 * t))
        es = split(extra)
        if pair < 2:
            y_ref[...] = 2.25 * y + dot3(split(y), es)
        if pair:
            z = z_ref[...]
            extra = 2.25 * z + identity * extra + dot3(es, split(z))
        z_ref[...] = extra
        identity = 2.25 * identity

    root = plus(identity, z_ref[...]) * (1.0 / jnp.sqrt(norm))
    projected = jnp.sum(proj_ref[...], axis=1, keepdims=True)
    once = jnp.sum(root * projected, axis=0, keepdims=True)
    once = jnp.broadcast_to(once, (8, MEMBERS)).T[:, 0:1]
    shift = jnp.sum(root * once, axis=0, keepdims=True)
    weights = split(root + shift)

    lane = lax.broadcasted_iota(jnp.int32, (MEMBERS, LANES), 1)
    low = (lane & 7) < 4
    even = (lane & 8) == 0

    def result_of(q, _):
        lanes = pl.ds(pl.multiple_of(q * LANES, LANES), LANES)
        cells = [
            jnp.concatenate([near[:, lanes], far[:, lanes]], axis=1)
            for near, far in ((ah_in_ref, ah_ref), (al_in_ref, al_ref))
        ]
        result = dot3(weights, cells)
        near = result[:, :LANES] + mean_in_ref[pl.ds(q, 1)]
        far = result[:, LANES:] + mean_ref[pl.ds(q, 1)]
        left = jnp.where(low, far, near)
        right = jnp.where(low, near, far)
        upper = jnp.where(even, left, pltpu.roll(right, 8, 1))
        lower = jnp.where(even, pltpu.roll(left, LANES - 8, 1), right)
        for strip, values in ((2 * q, upper), (2 * q + 1, lower)):
            place = strip_column(strip)
            for b in range(4):
                part = values[b * LANES : (b + 1) * LANES].reshape(2, 64, LANES)
                out_ref[pl.ds(place * 8 + ((b + place) & 3) * 2, 2)] = part
        return 0

    lax.fori_loop(0, 8, result_of, 0)


def vmem(count):
    return [pl.BlockSpec(memory_space=pltpu.VMEM) for _ in range(count)]


def in_vmem(x):
    return pltpu.with_memory_space_constraint(x, pltpu.VMEM)


def call(kernel, outs, scratch, limit, flops, name, *operands, specs=None):
    return pl.pallas_call(
        kernel,
        out_shape=[pltpu.VMEM(*out) for out in outs],
        in_specs=specs or vmem(len(operands)),
        out_specs=vmem(len(outs)),
        scratch_shapes=scratch,
        compiler_params=pltpu.CompilerParams(vmem_limit_bytes=limit * 2**20),
        cost_estimate=pl.CostEstimate(flops=flops, transcendentals=0, bytes_accessed=2**20),
        name=name,
    )(*operands)


def columns(count):
    return (64, count * 8, LANES), jnp.float32


def body(ensemble, obs_cells, obs_values, obs_rinv, obs_count):
    regions, block = ensemble.shape[0], ensemble.shape[1]
    following = OWNER[1:] + OWNER[:1]
    after = list(zip(OWNER, following))
    before = list(zip(following, OWNER))

    def exchange(x):
        return lax.all_to_all(x, MESH, split_axis=0, concat_axis=0, tiled=True, axis_index_groups=[OWNER])

    unit = 10**9

    slots = lax.broadcasted_iota(jnp.int32, obs_cells.shape, 1)
    active = (slots < obs_count[:, None]).astype(jnp.float32)
    rinv = obs_rinv * active / (MEMBERS - 1.0)
    grids = pl.pallas_call(
        obs_kernel, out_shape=pltpu.VMEM((32, LANES), jnp.float32), in_specs=vmem(3), out_specs=vmem(1)[0],
        compiler_params=pltpu.CompilerParams(vmem_limit_bytes=4 * 2**20), name="observations",
    )(obs_cells, rinv, obs_values)
    grids = lax.ppermute(grids, MESH, list(enumerate(OWNER)))
    pieces_in = exchange(ensemble.reshape(regions, block, LANES))
    pieces_in, grids = lax.optimization_barrier((pieces_in, grids))
    f32, bf16 = jnp.float32, jnp.bfloat16
    tiles, first, last = call(
        tiles_kernel, [columns(16), columns(HALO), columns(HALO)],
        [pltpu.VMEM((regions, block, LANES), f32), pltpu.SemaphoreType.DMA((16,))],
        8, unit, "tiles", pieces_in, specs=[pl.BlockSpec(memory_space=pl.ANY)],
    )
    west = lax.ppermute(last, MESH, after)
    east = lax.ppermute(first, MESH, before)
    *levels, inner = call(
        inner_kernel, [columns(14), columns(12), columns(10), columns(8)], [], 2, 4 * unit, "inner",
        in_vmem(tiles),
    )
    half = (MEMBERS, 1024), bf16
    square = (MEMBERS, MEMBERS), f32
    sums = (MEMBERS, LANES), f32
    means = (8, LANES), f32
    partial = call(
        inner_sums_kernel, [square, sums, means, half, half], [pltpu.VMEM(*half)] * 2,
        8, 6 * unit, "inner_sums", in_vmem(inner), in_vmem(grids),
    )
    inputs = [tiles, *levels, west, east, grids, *partial]
    (analysed,) = call(
        analysis_kernel,
        [((regions, block, LANES), f32)],
        [
            pltpu.VMEM(*shape)
            for shape in [columns(HALO)] * 6 + [columns(8), means] + [half] * 4 + [sums, square, square]
        ],
        24, 30 * unit, "analysis", *[in_vmem(x) for x in inputs],
    )
    return exchange(analysed).reshape(ensemble.shape)


def solution(mesh):
    return jax.shard_map(
        body,
        mesh=mesh,
        in_specs=(
            P(None, "mem", "space", None),
            P(("mem", "space"), None),
            P(("mem", "space"), None),
            P(("mem", "space"), None),
            P(("mem", "space")),
        ),
        out_specs=P(None, "mem", "space", None),
        check_vma=False,
    )
```

```python
import jax
import jax.numpy as jnp
from jax import lax
from jax.experimental import pallas as pl
from jax.experimental.pallas import tpu as pltpu
from jax.sharding import PartitionSpec as P

MEMBERS = 512
STEPS = 4
HALO = STEPS
LANES = 128
MESH = ("mem", "space")

def column_strip(place):
    return (place & 12) + ((place - (place >> 2)) & 3)


def strip_column(strip):
    return (strip & 12) + ((strip + (strip >> 2)) & 3)


OWNER = [
    (2 * ((k - place) & 3) + core) * 16 + column_strip(place)
    for place in range(16)
    for k in range(4)
    for core in range(2)
]


NT = (((1,), (1,)), ((), ()))


def split(x):
    high = x.astype(jnp.bfloat16)
    return high, (x - high.astype(jnp.float32)).astype(jnp.bfloat16)


def dot(a, b, dims=(((1,), (0,)), ((), ()))):
    return lax.dot_general(a, b, dims, preferred_element_type=jnp.float32)


def dot3(a, b):
    return dot(a[0], b[0]) + (dot(a[0], b[1]) + dot(a[1], b[0]))


def obs_kernel(cells_ref, rinv_ref, values_ref, out_ref):
    cells = cells_ref[...]
    slots = cells.shape[1]
    row, col = cells >> 4, cells & 15
    outer = ((col + 4) & 15) < 8
    place = (row >> 4) + jnp.where(outer, 8, 0)
    group = lax.broadcasted_iota(jnp.int32, (16, slots), 0) == place
    lane = lax.broadcasted_iota(jnp.int32, (LANES, slots), 0) == ((row & 7) * 2 + ((row >> 3) & 1)) * 8 + (col & 7)
    parts = []
    for value in (rinv_ref[...], rinv_ref[...] * values_ref[...]):
        for _ in range(3):
            part = value.astype(jnp.bfloat16).astype(jnp.float32)
            value = value - part
            parts.append(jnp.where(group, part, 0.0).astype(jnp.bfloat16))
    total = dot(jnp.concatenate(parts, axis=0), lane.astype(jnp.float32).astype(jnp.bfloat16), NT)
    out_ref[0:16] = total[0:16] + total[16:32] + total[32:48]
    out_ref[16:32] = total[48:64] + total[64:80] + total[80:96]


def at(col):
    return pl.ds(col * 8, 8)


def tiles_kernel(x_ref, u_ref, first_ref, last_ref, block_ref, sems):
    def arrival(s):
        part = pl.ds(s * 8, 8)
        return pltpu.make_async_copy(x_ref.at[part], block_ref.at[part], sems.at[s])

    for s in range(16):
        arrival(s).start()

    def column(place, _):
        s = column_strip(place)
        half = s // 8
        base = (s % 8) * 8
        arrival(place).wait()
        for b in range(4):
            block = block_ref[pl.ds(place * 8 + ((b + place) & 3) * 2, 2)].reshape(LANES, LANES)
            turned = (block * 0.5).T
            for j in range(8):
                for g in range(2):
                    u_ref[base + j, pl.ds(64 * g + half * 4 + b, 8, stride=8), :] = turned[
                        j * 16 + 8 * g : j * 16 + 8 * g + 8
                    ]
        return 0

    lax.fori_loop(0, 16, column, 0)

    def edge(r, _):
        first_ref[r] = u_ref[r, 0 : HALO * 8, :]
        last_ref[r] = u_ref[r, (16 - HALO) * 8 :, :]
        return 0

    lax.fori_loop(0, 64, edge, 0, unroll=4)


def sweep(load, store, groups, scale):
    columns = [k for group in groups for k in group]

    def row(r, n, c, s):
        first = 0
        for group in groups:
            last = first + len(group)
            around = [load(r, group[0] - 1), *c[first:last], load(r, group[-1] + 1)]
            for i, k in enumerate(group):
                at_k = c[first + i]
                p = around[i + 2] + s[first + i]
                q = around[i] + n[first + i]
                store(r, k, scale * ((at_k + (p + q)) - at_k * (p - q)))
            first = last

    def body(r, carry):
        n, c = carry
        s = tuple(load(r + 1, k) for k in columns)
        row(r, n, c, s)
        return c, s

    n = tuple(pltpu.roll(load(63, k), 4, 0) for k in columns)
    c = tuple(load(0, k) for k in columns)
    wrapped = tuple(pltpu.roll(t, 4, 0) for t in c)
    n, c = lax.fori_loop(0, 63, body, (n, c), unroll=3)
    row(63, n, c, wrapped)


def pieces(low, high, most):
    count = -(-(high - low) // most)
    edges = [low + (high - low) * i // count for i in range(count + 1)]
    return [list(range(a, b)) for a, b in zip(edges[:-1], edges[1:])]


def scale_of(step):
    return 0.4 if step == STEPS - 1 else 0.2


def inner_kernel(u_ref, one_ref, two_ref, three_ref, inner_ref):
    levels = [u_ref, one_ref, two_ref, three_ref]
    for step in range(STEPS):
        low, high = step + 1, 15 - step

        def load(r, col, step=step):
            return levels[step][r, at(col - step), :]

        def store(r, col, value, step=step, low=low):
            if step < STEPS - 1:
                levels[step + 1][r, at(col - low), :] = value
            else:
                inner_ref[r, at(col & 7), :] = value

        for columns in pieces(low, high, 8):
            sweep(load, store, [columns], scale_of(step))


def outer_forecast(levels, west_ref, east_ref, wests, easts, outer_ref):
    for step in range(STEPS):
        reach = HALO - step

        def load(r, col, step=step, reach=reach):
            if step == 0:
                if col < 0:
                    return west_ref[r, at(col + HALO), :]
                if col >= 16:
                    return east_ref[r, at(col - 16), :]
            elif col < step:
                return wests[step - 1][r, at(col + reach), :]
            elif col >= 16 - step:
                return easts[step - 1][r, at(col - 16 + step), :]
            return levels[step][r, at(col - step), :]

        def store(r, col, value, step=step, reach=reach):
            if step == STEPS - 1:
                outer_ref[r, at(col & 7), :] = value
            elif col < 8:
                wests[step][r, at(col + reach - 1), :] = value
            else:
                easts[step][r, at(col - 15 + step), :] = value

        sides = [list(range(1 - reach, step + 1)), list(range(15 - step, 15 + reach))]
        sweep(load, store, sides, scale_of(step))


def gather_groups(part_ref, obs_ref, first_group, mean_ref, ah_ref, al_ref, bh_ref, bl_ref, proj_ref):
    def group(q, _):
        half = q // 4
        base = (q % 4) * 16
        blocks = []
        for b in range(4):
            place = pl.ds(half * 4 + b, 8, stride=8)
            rows = [part_ref[base + 8 * p + j, place, :] for j in range(8) for p in range(2)]
            blocks.append(jnp.concatenate(rows, axis=0).T)
        total = blocks[0] + blocks[1] + blocks[2] + blocks[3]
        mean = jnp.sum(total, axis=0, keepdims=True) * (1.0 / MEMBERS)
        mean_ref[pl.ds(q, 1)] = mean
        weight = obs_ref[pl.ds(first_group + q, 1)]
        root = jnp.sqrt(weight)
        misfit = obs_ref[pl.ds(first_group + q + 16, 1)] - weight * mean
        lanes = pl.ds(pl.multiple_of(q * LANES, LANES), LANES)
        for b in range(4):
            part = pl.ds(b * LANES, LANES)
            anomaly = blocks[b] - mean
            ah_ref[part, lanes], al_ref[part, lanes] = split(anomaly)
            bh_ref[part, lanes], bl_ref[part, lanes] = split(anomaly * root)
            proj_ref[part] += anomaly * misfit
        return 0

    lax.fori_loop(0, 8, group, 0)
    high, low = bh_ref[...], bl_ref[...]
    cross = dot(high, low, NT)
    return dot(high, high, NT) + (cross + cross.T)


def inner_sums_kernel(inner_ref, obs_ref, matrix_ref, proj_ref, mean_ref, ah_ref, al_ref, bh_ref, bl_ref):
    proj_ref[...] = jnp.zeros_like(proj_ref)
    matrix_ref[...] = gather_groups(
        inner_ref, obs_ref, 0, mean_ref, ah_ref, al_ref, bh_ref, bl_ref, proj_ref
    )


def analysis_kernel(
    u_ref, one_ref, two_ref, three_ref, west_ref, east_ref, obs_ref,
    matrix_ref, sums_ref, mean_in_ref, ah_in_ref, al_in_ref,
    out_ref,
    w1_ref, w2_ref, w3_ref, e1_ref, e2_ref, e3_ref, outer_ref,
    mean_ref, ah_ref, al_ref, bh_ref, bl_ref, proj_ref, y_ref, z_ref,
):
    outer_forecast(
        [u_ref, one_ref, two_ref, three_ref], west_ref, east_ref,
        [w1_ref, w2_ref, w3_ref], [e1_ref, e2_ref, e3_ref], outer_ref,
    )
    proj_ref[...] = sums_ref[...]
    matrix = matrix_ref[...] + gather_groups(
        outer_ref, obs_ref, 8, mean_ref, ah_ref, al_ref, bh_ref, bl_ref, proj_ref
    )

    shape = (MEMBERS, MEMBERS)
    diagonal = lax.broadcasted_iota(jnp.int32, shape, 0) == lax.broadcasted_iota(jnp.int32, shape, 1)

    def plus(coefficient, x):
        return x + jnp.where(diagonal, coefficient, 0.0)

    matrix = plus(1.0, matrix)
    norm = jnp.sqrt(jnp.sum(jnp.sum(matrix * matrix, axis=0, keepdims=True), axis=1, keepdims=True))
    y_ref[...] = matrix * (1.0 / norm)

    identity = 1.0
    for pair in range(3):
        y = y_ref[...]
        t = y
        if pair:
            t = identity * y + dot3(split(z_ref[...]), split(y))
        ts = split(t)
        square = dot3(ts, ts)
        extra = 1.6875 * square - 2.4375 * t + dot3(split(square), split(0.0625 * square - 0.5625 * t))
        es = split(extra)
        if pair < 2:
            y_ref[...] = 2.25 * y + dot3(split(y), es)
        if pair:
            z = z_ref[...]
            extra = 2.25 * z + identity * extra + dot3(es, split(z))
        z_ref[...] = extra
        identity = 2.25 * identity

    root = plus(identity, z_ref[...]) * (1.0 / jnp.sqrt(norm))
    projected = jnp.sum(proj_ref[...], axis=1, keepdims=True)
    once = jnp.sum(root * projected, axis=0, keepdims=True)
    once = jnp.broadcast_to(once, (8, MEMBERS)).T[:, 0:1]
    shift = jnp.sum(root * once, axis=0, keepdims=True)
    weights = split(root + shift)

    lane = lax.broadcasted_iota(jnp.int32, (MEMBERS, LANES), 1)
    low = (lane & 7) < 4
    even = (lane & 8) == 0

    def result_of(q, _):
        lanes = pl.ds(pl.multiple_of(q * LANES, LANES), LANES)
        cells = [
            jnp.concatenate([near[:, lanes], far[:, lanes]], axis=1)
            for near, far in ((ah_in_ref, ah_ref), (al_in_ref, al_ref))
        ]
        result = dot3(weights, cells)
        near = result[:, :LANES] + mean_in_ref[pl.ds(q, 1)]
        far = result[:, LANES:] + mean_ref[pl.ds(q, 1)]
        left = jnp.where(low, far, near)
        right = jnp.where(low, near, far)
        upper = jnp.where(even, left, pltpu.roll(right, 8, 1))
        lower = jnp.where(even, pltpu.roll(left, LANES - 8, 1), right)
        for strip, values in ((2 * q, upper), (2 * q + 1, lower)):
            place = strip_column(strip)
            for b in range(4):
                part = values[b * LANES : (b + 1) * LANES].reshape(2, 64, LANES)
                out_ref[pl.ds(place * 8 + ((b + place) & 3) * 2, 2)] = part
        return 0

    lax.fori_loop(0, 8, result_of, 0, unroll=2)


def vmem(count):
    return [pl.BlockSpec(memory_space=pltpu.VMEM) for _ in range(count)]


def in_vmem(x):
    return pltpu.with_memory_space_constraint(x, pltpu.VMEM)


def call(kernel, outs, scratch, limit, flops, name, *operands, specs=None):
    return pl.pallas_call(
        kernel,
        out_shape=[pltpu.VMEM(*out) for out in outs],
        in_specs=specs or vmem(len(operands)),
        out_specs=vmem(len(outs)),
        scratch_shapes=scratch,
        compiler_params=pltpu.CompilerParams(vmem_limit_bytes=limit * 2**20),
        cost_estimate=pl.CostEstimate(flops=flops, transcendentals=0, bytes_accessed=2**20),
        name=name,
    )(*operands)


def columns(count):
    return (64, count * 8, LANES), jnp.float32


def body(ensemble, obs_cells, obs_values, obs_rinv, obs_count):
    regions, block = ensemble.shape[0], ensemble.shape[1]
    following = OWNER[1:] + OWNER[:1]
    after = list(zip(OWNER, following))
    before = list(zip(following, OWNER))

    def exchange(x):
        return lax.all_to_all(x, MESH, split_axis=0, concat_axis=0, tiled=True, axis_index_groups=[OWNER])

    unit = 10**9

    slots = lax.broadcasted_iota(jnp.int32, obs_cells.shape, 1)
    active = (slots < obs_count[:, None]).astype(jnp.float32)
    rinv = obs_rinv * active / (MEMBERS - 1.0)
    grids = pl.pallas_call(
        obs_kernel, out_shape=pltpu.VMEM((32, LANES), jnp.float32), in_specs=vmem(3), out_specs=vmem(1)[0],
        compiler_params=pltpu.CompilerParams(vmem_limit_bytes=4 * 2**20), name="observations",
    )(obs_cells, rinv, obs_values)
    grids = lax.ppermute(grids, MESH, list(enumerate(OWNER)))
    pieces_in = exchange(ensemble.reshape(regions, block, LANES))
    pieces_in, grids = lax.optimization_barrier((pieces_in, grids))
    f32, bf16 = jnp.float32, jnp.bfloat16
    tiles, first, last = call(
        tiles_kernel, [columns(16), columns(HALO), columns(HALO)],
        [pltpu.VMEM((regions, block, LANES), f32), pltpu.SemaphoreType.DMA((16,))],
        8, unit, "tiles", pieces_in, specs=[pl.BlockSpec(memory_space=pl.ANY)],
    )
    west = lax.ppermute(last, MESH, after)
    east = lax.ppermute(first, MESH, before)
    *levels, inner = call(
        inner_kernel, [columns(14), columns(12), columns(10), columns(8)], [], 2, 4 * unit, "inner",
        in_vmem(tiles),
    )
    half = (MEMBERS, 1024), bf16
    square = (MEMBERS, MEMBERS), f32
    sums = (MEMBERS, LANES), f32
    means = (8, LANES), f32
    partial = call(
        inner_sums_kernel, [square, sums, means, half, half], [pltpu.VMEM(*half)] * 2,
        8, 6 * unit, "inner_sums", in_vmem(inner), in_vmem(grids),
    )
    inputs = [tiles, *levels, west, east, grids, *partial]
    (analysed,) = call(
        analysis_kernel,
        [((regions, block, LANES), f32)],
        [
            pltpu.VMEM(*shape)
            for shape in [columns(HALO)] * 6 + [columns(8), means] + [half] * 4 + [sums, square, square]
        ],
        24, 30 * unit, "analysis", *[in_vmem(x) for x in inputs],
    )
    return exchange(analysed).reshape(ensemble.shape)


def solution(mesh):
    return jax.shard_map(
        body,
        mesh=mesh,
        in_specs=(
            P(None, "mem", "space", None),
            P(("mem", "space"), None),
            P(("mem", "space"), None),
            P(("mem", "space"), None),
            P(("mem", "space")),
        ),
        out_specs=P(None, "mem", "space", None),
        check_vma=False,
    )
```

```python
import jax
import jax.numpy as jnp
from jax import lax
from jax.experimental import pallas as pl
from jax.experimental.pallas import tpu as pltpu
from jax.sharding import PartitionSpec as P

MEMBERS = 512
STEPS = 4
HALO = STEPS
LANES = 128
MESH = ("mem", "space")

def column_strip(place):
    return (place & 12) + ((place - (place >> 2)) & 3)


def strip_column(strip):
    return (strip & 12) + ((strip + (strip >> 2)) & 3)


OWNER = [
    (2 * ((k - place) & 3) + core) * 16 + column_strip(place)
    for place in range(16)
    for k in range(4)
    for core in range(2)
]


NT = (((1,), (1,)), ((), ()))


def split(x):
    high = x.astype(jnp.bfloat16)
    return high, (x - high.astype(jnp.float32)).astype(jnp.bfloat16)


def dot(a, b, dims=(((1,), (0,)), ((), ()))):
    return lax.dot_general(a, b, dims, preferred_element_type=jnp.float32)


def dot3(a, b):
    return dot(a[0], b[0]) + (dot(a[0], b[1]) + dot(a[1], b[0]))


def symmetric3(a, b):
    middle = MEMBERS // 2
    top = dot3([x[:middle] for x in a], b)
    corner = dot3([x[middle:] for x in a], [x[:, middle:] for x in b])
    bottom = jnp.concatenate([top[:, middle:].T, corner], axis=1)
    return jnp.concatenate([top, bottom], axis=0)


def obs_kernel(cells_ref, rinv_ref, values_ref, out_ref):
    cells = cells_ref[...]
    slots = cells.shape[1]
    row, col = cells >> 4, cells & 15
    outer = ((col + 4) & 15) < 8
    place = (row >> 4) + jnp.where(outer, 8, 0)
    group = lax.broadcasted_iota(jnp.int32, (16, slots), 0) == place
    lane = lax.broadcasted_iota(jnp.int32, (LANES, slots), 0) == ((row & 7) * 2 + ((row >> 3) & 1)) * 8 + (col & 7)
    parts = []
    for value in (rinv_ref[...], rinv_ref[...] * values_ref[...]):
        for _ in range(3):
            part = value.astype(jnp.bfloat16).astype(jnp.float32)
            value = value - part
            parts.append(jnp.where(group, part, 0.0).astype(jnp.bfloat16))
    total = dot(jnp.concatenate(parts, axis=0), lane.astype(jnp.float32).astype(jnp.bfloat16), NT)
    out_ref[0:16] = total[0:16] + total[16:32] + total[32:48]
    out_ref[16:32] = total[48:64] + total[64:80] + total[80:96]


def at(col):
    return pl.ds(col * 8, 8)


def tiles_kernel(x_ref, u_ref, first_ref, last_ref, block_ref, sems):
    def arrival(s):
        part = pl.ds(s * 8, 8)
        return pltpu.make_async_copy(x_ref.at[part], block_ref.at[part], sems.at[s])

    for s in range(16):
        arrival(s).start()

    def column(place, _):
        s = column_strip(place)
        half = s // 8
        base = (s % 8) * 8
        arrival(place).wait()
        for b in range(4):
            block = block_ref[pl.ds(place * 8 + ((b + place) & 3) * 2, 2)].reshape(LANES, LANES)
            turned = (block * 0.5).T
            for j in range(8):
                for g in range(2):
                    u_ref[base + j, pl.ds(64 * g + half * 4 + b, 8, stride=8), :] = turned[
                        j * 16 + 8 * g : j * 16 + 8 * g + 8
                    ]
        return 0

    lax.fori_loop(0, 16, column, 0)

    def edge(r, _):
        first_ref[r] = u_ref[r, 0 : HALO * 8, :]
        last_ref[r] = u_ref[r, (16 - HALO) * 8 :, :]
        return 0

    lax.fori_loop(0, 64, edge, 0, unroll=4)


def sweep(load, store, groups, scale):
    columns = [k for group in groups for k in group]

    def row(r, n, c, s):
        first = 0
        for group in groups:
            last = first + len(group)
            around = [load(r, group[0] - 1), *c[first:last], load(r, group[-1] + 1)]
            for i, k in enumerate(group):
                at_k = c[first + i]
                p = around[i + 2] + s[first + i]
                q = around[i] + n[first + i]
                store(r, k, scale * ((at_k + (p + q)) - at_k * (p - q)))
            first = last

    def body(r, carry):
        n, c = carry
        s = tuple(load(r + 1, k) for k in columns)
        row(r, n, c, s)
        return c, s

    n = tuple(pltpu.roll(load(63, k), 4, 0) for k in columns)
    c = tuple(load(0, k) for k in columns)
    wrapped = tuple(pltpu.roll(t, 4, 0) for t in c)
    n, c = lax.fori_loop(0, 63, body, (n, c), unroll=3)
    row(63, n, c, wrapped)


def pieces(low, high, most):
    count = -(-(high - low) // most)
    edges = [low + (high - low) * i // count for i in range(count + 1)]
    return [list(range(a, b)) for a, b in zip(edges[:-1], edges[1:])]


def scale_of(step):
    return 0.4 if step == STEPS - 1 else 0.2


def inner_kernel(u_ref, one_ref, two_ref, three_ref, inner_ref):
    levels = [u_ref, one_ref, two_ref, three_ref]
    for step in range(STEPS):
        low, high = step + 1, 15 - step

        def load(r, col, step=step):
            return levels[step][r, at(col - step), :]

        def store(r, col, value, step=step, low=low):
            if step < STEPS - 1:
                levels[step + 1][r, at(col - low), :] = value
            else:
                inner_ref[r, at(col & 7), :] = value

        for columns in pieces(low, high, 8):
            sweep(load, store, [columns], scale_of(step))


def outer_forecast(levels, west_ref, east_ref, wests, easts, outer_ref):
    for step in range(STEPS):
        reach = HALO - step

        def load(r, col, step=step, reach=reach):
            if step == 0:
                if col < 0:
                    return west_ref[r, at(col + HALO), :]
                if col >= 16:
                    return east_ref[r, at(col - 16), :]
            elif col < step:
                return wests[step - 1][r, at(col + reach), :]
            elif col >= 16 - step:
                return easts[step - 1][r, at(col - 16 + step), :]
            return levels[step][r, at(col - step), :]

        def store(r, col, value, step=step, reach=reach):
            if step == STEPS - 1:
                outer_ref[r, at(col & 7), :] = value
            elif col < 8:
                wests[step][r, at(col + reach - 1), :] = value
            else:
                easts[step][r, at(col - 15 + step), :] = value

        sides = [list(range(1 - reach, step + 1)), list(range(15 - step, 15 + reach))]
        sweep(load, store, sides, scale_of(step))


def gather_groups(part_ref, obs_ref, first_group, mean_ref, ah_ref, al_ref, bh_ref, bl_ref, proj_ref):
    def group(q, _):
        half = q // 4
        base = (q % 4) * 16
        blocks = []
        for b in range(4):
            place = pl.ds(half * 4 + b, 8, stride=8)
            rows = [part_ref[base + 8 * p + j, place, :] for j in range(8) for p in range(2)]
            blocks.append(jnp.concatenate(rows, axis=0).T)
        total = blocks[0] + blocks[1] + blocks[2] + blocks[3]
        mean = jnp.sum(total, axis=0, keepdims=True) * (1.0 / MEMBERS)
        mean_ref[pl.ds(q, 1)] = mean
        weight = obs_ref[pl.ds(first_group + q, 1)]
        root = jnp.sqrt(weight)
        misfit = obs_ref[pl.ds(first_group + q + 16, 1)] - weight * mean
        lanes = pl.ds(pl.multiple_of(q * LANES, LANES), LANES)
        for b in range(4):
            part = pl.ds(b * LANES, LANES)
            anomaly = blocks[b] - mean
            ah_ref[part, lanes], al_ref[part, lanes] = split(anomaly)
            bh_ref[part, lanes], bl_ref[part, lanes] = split(anomaly * root)
            proj_ref[part] += anomaly * misfit
        return 0

    lax.fori_loop(0, 8, group, 0)
    high, low = bh_ref[...], bl_ref[...]
    cross = dot(high, low, NT)
    return dot(high, high, NT) + (cross + cross.T)


def inner_sums_kernel(inner_ref, obs_ref, matrix_ref, proj_ref, mean_ref, ah_ref, al_ref, bh_ref, bl_ref):
    proj_ref[...] = jnp.zeros_like(proj_ref)
    matrix_ref[...] = gather_groups(
        inner_ref, obs_ref, 0, mean_ref, ah_ref, al_ref, bh_ref, bl_ref, proj_ref
    )


def analysis_kernel(
    u_ref, one_ref, two_ref, three_ref, west_ref, east_ref, obs_ref,
    matrix_ref, sums_ref, mean_in_ref, ah_in_ref, al_in_ref,
    out_ref,
    w1_ref, w2_ref, w3_ref, e1_ref, e2_ref, e3_ref, outer_ref,
    mean_ref, ah_ref, al_ref, bh_ref, bl_ref, proj_ref, y_ref, z_ref,
):
    outer_forecast(
        [u_ref, one_ref, two_ref, three_ref], west_ref, east_ref,
        [w1_ref, w2_ref, w3_ref], [e1_ref, e2_ref, e3_ref], outer_ref,
    )
    proj_ref[...] = sums_ref[...]
    matrix = matrix_ref[...] + gather_groups(
        outer_ref, obs_ref, 8, mean_ref, ah_ref, al_ref, bh_ref, bl_ref, proj_ref
    )

    shape = (MEMBERS, MEMBERS)
    diagonal = lax.broadcasted_iota(jnp.int32, shape, 0) == lax.broadcasted_iota(jnp.int32, shape, 1)

    def plus(coefficient, x):
        return x + jnp.where(diagonal, coefficient, 0.0)

    matrix = plus(1.0, matrix)
    norm = jnp.sqrt(jnp.sum(jnp.sum(matrix * matrix, axis=0, keepdims=True), axis=1, keepdims=True))
    y_ref[...] = matrix * (1.0 / norm)

    identity = 1.0
    for pair in range(3):
        y = y_ref[...]
        t = y
        if pair:
            t = identity * y + symmetric3(split(z_ref[...]), split(y))
        ts = split(t)
        square = symmetric3(ts, ts)
        extra = 1.6875 * square - 2.4375 * t + symmetric3(split(square), split(0.0625 * square - 0.5625 * t))
        es = split(extra)
        if pair < 2:
            y_ref[...] = 2.25 * y + symmetric3(split(y), es)
        if pair:
            z = z_ref[...]
            extra = 2.25 * z + identity * extra + symmetric3(es, split(z))
        z_ref[...] = extra
        identity = 2.25 * identity

    root = plus(identity, z_ref[...]) * (1.0 / jnp.sqrt(norm))
    projected = jnp.sum(proj_ref[...], axis=1, keepdims=True)
    once = jnp.sum(root * projected, axis=0, keepdims=True)
    once = jnp.broadcast_to(once, (8, MEMBERS)).T[:, 0:1]
    shift = jnp.sum(root * once, axis=0, keepdims=True)
    weights = split(root + shift)

    lane = lax.broadcasted_iota(jnp.int32, (MEMBERS, LANES), 1)
    low = (lane & 7) < 4
    even = (lane & 8) == 0

    def result_of(q, _):
        lanes = pl.ds(pl.multiple_of(q * LANES, LANES), LANES)
        cells = [
            jnp.concatenate([near[:, lanes], far[:, lanes]], axis=1)
            for near, far in ((ah_in_ref, ah_ref), (al_in_ref, al_ref))
        ]
        result = dot3(weights, cells)
        near = result[:, :LANES] + mean_in_ref[pl.ds(q, 1)]
        far = result[:, LANES:] + mean_ref[pl.ds(q, 1)]
        left = jnp.where(low, far, near)
        right = jnp.where(low, near, far)
        upper = jnp.where(even, left, pltpu.roll(right, 8, 1))
        lower = jnp.where(even, pltpu.roll(left, LANES - 8, 1), right)
        for strip, values in ((2 * q, upper), (2 * q + 1, lower)):
            place = strip_column(strip)
            for b in range(4):
                part = values[b * LANES : (b + 1) * LANES].reshape(2, 64, LANES)
                out_ref[pl.ds(place * 8 + ((b + place) & 3) * 2, 2)] = part
        return 0

    lax.fori_loop(0, 8, result_of, 0, unroll=2)


def vmem(count):
    return [pl.BlockSpec(memory_space=pltpu.VMEM) for _ in range(count)]


def in_vmem(x):
    return pltpu.with_memory_space_constraint(x, pltpu.VMEM)


def call(kernel, outs, scratch, limit, flops, name, *operands, specs=None):
    return pl.pallas_call(
        kernel,
        out_shape=[pltpu.VMEM(*out) for out in outs],
        in_specs=specs or vmem(len(operands)),
        out_specs=vmem(len(outs)),
        scratch_shapes=scratch,
        compiler_params=pltpu.CompilerParams(vmem_limit_bytes=limit * 2**20),
        cost_estimate=pl.CostEstimate(flops=flops, transcendentals=0, bytes_accessed=2**20),
        name=name,
    )(*operands)


def columns(count):
    return (64, count * 8, LANES), jnp.float32


def body(ensemble, obs_cells, obs_values, obs_rinv, obs_count):
    regions, block = ensemble.shape[0], ensemble.shape[1]
    following = OWNER[1:] + OWNER[:1]
    after = list(zip(OWNER, following))
    before = list(zip(following, OWNER))

    def exchange(x):
        return lax.all_to_all(x, MESH, split_axis=0, concat_axis=0, tiled=True, axis_index_groups=[OWNER])

    unit = 10**9

    slots = lax.broadcasted_iota(jnp.int32, obs_cells.shape, 1)
    active = (slots < obs_count[:, None]).astype(jnp.float32)
    rinv = obs_rinv * active / (MEMBERS - 1.0)
    grids = pl.pallas_call(
        obs_kernel, out_shape=pltpu.VMEM((32, LANES), jnp.float32), in_specs=vmem(3), out_specs=vmem(1)[0],
        compiler_params=pltpu.CompilerParams(vmem_limit_bytes=4 * 2**20), name="observations",
    )(obs_cells, rinv, obs_values)
    grids = lax.ppermute(grids, MESH, list(enumerate(OWNER)))
    pieces_in = exchange(ensemble.reshape(regions, block, LANES))
    pieces_in, grids = lax.optimization_barrier((pieces_in, grids))
    f32, bf16 = jnp.float32, jnp.bfloat16
    tiles, first, last = call(
        tiles_kernel, [columns(16), columns(HALO), columns(HALO)],
        [pltpu.VMEM((regions, block, LANES), f32), pltpu.SemaphoreType.DMA((16,))],
        8, unit, "tiles", pieces_in, specs=[pl.BlockSpec(memory_space=pl.ANY)],
    )
    west = lax.ppermute(last, MESH, after)
    east = lax.ppermute(first, MESH, before)
    *levels, inner = call(
        inner_kernel, [columns(14), columns(12), columns(10), columns(8)], [], 2, 4 * unit, "inner",
        in_vmem(tiles),
    )
    half = (MEMBERS, 1024), bf16
    square = (MEMBERS, MEMBERS), f32
    sums = (MEMBERS, LANES), f32
    means = (8, LANES), f32
    partial = call(
        inner_sums_kernel, [square, sums, means, half, half], [pltpu.VMEM(*half)] * 2,
        8, 6 * unit, "inner_sums", in_vmem(inner), in_vmem(grids),
    )
    inputs = [tiles, *levels, west, east, grids, *partial]
    (analysed,) = call(
        analysis_kernel,
        [((regions, block, LANES), f32)],
        [
            pltpu.VMEM(*shape)
            for shape in [columns(HALO)] * 6 + [columns(8), means] + [half] * 4 + [sums, square, square]
        ],
        24, 30 * unit, "analysis", *[in_vmem(x) for x in inputs],
    )
    return exchange(analysed).reshape(ensemble.shape)


def solution(mesh):
    return jax.shard_map(
        body,
        mesh=mesh,
        in_specs=(
            P(None, "mem", "space", None),
            P(("mem", "space"), None),
            P(("mem", "space"), None),
            P(("mem", "space"), None),
            P(("mem", "space")),
        ),
        out_specs=P(None, "mem", "space", None),
        check_vma=False,
    )
```

```python
import jax
import jax.numpy as jnp
from jax import lax
from jax.experimental import pallas as pl
from jax.experimental.pallas import tpu as pltpu
from jax.sharding import PartitionSpec as P

MEMBERS = 512
STEPS = 4
HALO = STEPS
LANES = 128
MESH = ("mem", "space")

def column_strip(place):
    return (place & 12) + ((place - (place >> 2)) & 3)


def strip_column(strip):
    return (strip & 12) + ((strip + (strip >> 2)) & 3)


OWNER = [
    (2 * ((k - place) & 3) + core) * 16 + column_strip(place)
    for place in range(16)
    for k in range(4)
    for core in range(2)
]


NT = (((1,), (1,)), ((), ()))


def split(x):
    high = x.astype(jnp.bfloat16)
    return high, (x - high.astype(jnp.float32)).astype(jnp.bfloat16)


def dot(a, b, dims=(((1,), (0,)), ((), ()))):
    return lax.dot_general(a, b, dims, preferred_element_type=jnp.float32)


def dot3(a, b):
    return dot(a[0], b[0]) + (dot(a[0], b[1]) + dot(a[1], b[0]))


def symmetric3(a, b):
    middle = MEMBERS // 2
    top = dot3([x[:middle] for x in a], b)
    corner = dot3([x[middle:] for x in a], [x[:, middle:] for x in b])
    bottom = jnp.concatenate([top[:, middle:].T, corner], axis=1)
    return jnp.concatenate([top, bottom], axis=0)


def obs_kernel(cells_ref, rinv_ref, values_ref, out_ref):
    cells = cells_ref[...]
    slots = cells.shape[1]
    row, col = cells >> 4, cells & 15
    outer = ((col + 4) & 15) < 8
    place = (row >> 4) + jnp.where(outer, 8, 0)
    group = lax.broadcasted_iota(jnp.int32, (16, slots), 0) == place
    lane = lax.broadcasted_iota(jnp.int32, (LANES, slots), 0) == ((row & 7) * 2 + ((row >> 3) & 1)) * 8 + (col & 7)
    parts = []
    for value in (rinv_ref[...], rinv_ref[...] * values_ref[...]):
        for _ in range(3):
            part = value.astype(jnp.bfloat16).astype(jnp.float32)
            value = value - part
            parts.append(jnp.where(group, part, 0.0).astype(jnp.bfloat16))
    total = dot(jnp.concatenate(parts, axis=0), lane.astype(jnp.float32).astype(jnp.bfloat16), NT)
    out_ref[0:16] = total[0:16] + total[16:32] + total[32:48]
    out_ref[16:32] = total[48:64] + total[64:80] + total[80:96]


def at(col):
    return pl.ds(col * 8, 8)


def tiles_kernel(x_ref, u_ref, first_ref, last_ref, block_ref, sems):
    def arrival(s):
        part = pl.ds(s * 8, 8)
        return pltpu.make_async_copy(x_ref.at[part], block_ref.at[part], sems.at[s])

    for s in range(16):
        arrival(s).start()

    def column(place, _):
        s = column_strip(place)
        half = s // 8
        base = (s % 8) * 8
        arrival(place).wait()
        for b in range(4):
            block = block_ref[pl.ds(place * 8 + ((b + place) & 3) * 2, 2)].reshape(LANES, LANES)
            turned = (block * 0.5).T
            for j in range(8):
                for g in range(2):
                    u_ref[base + j, pl.ds(64 * g + half * 4 + b, 8, stride=8), :] = turned[
                        j * 16 + 8 * g : j * 16 + 8 * g + 8
                    ]
        return 0

    lax.fori_loop(0, 16, column, 0)

    def edge(r, _):
        first_ref[r] = u_ref[r, 0 : HALO * 8, :]
        last_ref[r] = u_ref[r, (16 - HALO) * 8 :, :]
        return 0

    lax.fori_loop(0, 64, edge, 0, unroll=4)


def sweep(load, store, groups, scale):
    columns = [k for group in groups for k in group]

    def row(r, n, c, s):
        first = 0
        for group in groups:
            last = first + len(group)
            around = [load(r, group[0] - 1), *c[first:last], load(r, group[-1] + 1)]
            for i, k in enumerate(group):
                at_k = c[first + i]
                p = around[i + 2] + s[first + i]
                q = around[i] + n[first + i]
                store(r, k, scale * ((at_k + (p + q)) - at_k * (p - q)))
            first = last

    def body(r, carry):
        n, c = carry
        s = tuple(load(r + 1, k) for k in columns)
        row(r, n, c, s)
        return c, s

    n = tuple(pltpu.roll(load(63, k), 4, 0) for k in columns)
    c = tuple(load(0, k) for k in columns)
    wrapped = tuple(pltpu.roll(t, 4, 0) for t in c)
    n, c = lax.fori_loop(0, 63, body, (n, c), unroll=3)
    row(63, n, c, wrapped)


def pieces(low, high, most):
    count = -(-(high - low) // most)
    edges = [low + (high - low) * i // count for i in range(count + 1)]
    return [list(range(a, b)) for a, b in zip(edges[:-1], edges[1:])]


def scale_of(step):
    return 0.4 if step == STEPS - 1 else 0.2


def inner_kernel(u_ref, one_ref, two_ref, three_ref, inner_ref):
    levels = [u_ref, one_ref, two_ref, three_ref]
    for step in range(STEPS):
        low, high = step + 1, 15 - step

        def load(r, col, step=step):
            return levels[step][r, at(col - step), :]

        def store(r, col, value, step=step, low=low):
            if step < STEPS - 1:
                levels[step + 1][r, at(col - low), :] = value
            else:
                inner_ref[r, at(col & 7), :] = value

        for columns in pieces(low, high, 8):
            sweep(load, store, [columns], scale_of(step))


def outer_forecast(levels, west_ref, east_ref, wests, easts, outer_ref):
    for step in range(STEPS):
        reach = HALO - step

        def load(r, col, step=step, reach=reach):
            if step == 0:
                if col < 0:
                    return west_ref[r, at(col + HALO), :]
                if col >= 16:
                    return east_ref[r, at(col - 16), :]
            elif col < step:
                return wests[step - 1][r, at(col + reach), :]
            elif col >= 16 - step:
                return easts[step - 1][r, at(col - 16 + step), :]
            return levels[step][r, at(col - step), :]

        def store(r, col, value, step=step, reach=reach):
            if step == STEPS - 1:
                outer_ref[r, at(col & 7), :] = value
            elif col < 8:
                wests[step][r, at(col + reach - 1), :] = value
            else:
                easts[step][r, at(col - 15 + step), :] = value

        sides = [list(range(1 - reach, step + 1)), list(range(15 - step, 15 + reach))]
        sweep(load, store, sides, scale_of(step))


def gather_groups(part_ref, obs_ref, first_group, mean_ref, ah_ref, al_ref, bh_ref, bl_ref, proj_ref):
    def group(q, _):
        half = q // 4
        base = (q % 4) * 16
        blocks = []
        for b in range(4):
            place = pl.ds(half * 4 + b, 8, stride=8)
            rows = [part_ref[base + 8 * p + j, place, :] for j in range(8) for p in range(2)]
            blocks.append(jnp.concatenate(rows, axis=0).T)
        total = blocks[0] + blocks[1] + blocks[2] + blocks[3]
        mean = jnp.sum(total, axis=0, keepdims=True) * (1.0 / MEMBERS)
        mean_ref[pl.ds(q, 1)] = mean
        weight = obs_ref[pl.ds(first_group + q, 1)]
        root = jnp.sqrt(weight)
        misfit = obs_ref[pl.ds(first_group + q + 16, 1)] - weight * mean
        lanes = pl.ds(pl.multiple_of(q * LANES, LANES), LANES)
        for b in range(4):
            part = pl.ds(b * LANES, LANES)
            anomaly = blocks[b] - mean
            ah_ref[part, lanes], al_ref[part, lanes] = split(anomaly)
            bh_ref[part, lanes], bl_ref[part, lanes] = split(anomaly * root)
            proj_ref[part] += anomaly * misfit
        return 0

    lax.fori_loop(0, 8, group, 0)
    high, low = bh_ref[...], bl_ref[...]
    cross = dot(high, low, NT)
    return dot(high, high, NT) + (cross + cross.T)


def inner_sums_kernel(inner_ref, obs_ref, matrix_ref, proj_ref, mean_ref, ah_ref, al_ref, bh_ref, bl_ref):
    proj_ref[...] = jnp.zeros_like(proj_ref)
    matrix_ref[...] = gather_groups(
        inner_ref, obs_ref, 0, mean_ref, ah_ref, al_ref, bh_ref, bl_ref, proj_ref
    )


def analysis_kernel(
    u_ref, one_ref, two_ref, three_ref, west_ref, east_ref, obs_ref,
    matrix_ref, sums_ref, mean_in_ref, ah_in_ref, al_in_ref,
    out_ref,
    w1_ref, w2_ref, w3_ref, e1_ref, e2_ref, e3_ref, outer_ref,
    mean_ref, ah_ref, al_ref, bh_ref, bl_ref, proj_ref, y_ref, z_ref,
):
    outer_forecast(
        [u_ref, one_ref, two_ref, three_ref], west_ref, east_ref,
        [w1_ref, w2_ref, w3_ref], [e1_ref, e2_ref, e3_ref], outer_ref,
    )
    proj_ref[...] = sums_ref[...]
    matrix = matrix_ref[...] + gather_groups(
        outer_ref, obs_ref, 8, mean_ref, ah_ref, al_ref, bh_ref, bl_ref, proj_ref
    )

    shape = (MEMBERS, MEMBERS)
    diagonal = lax.broadcasted_iota(jnp.int32, shape, 0) == lax.broadcasted_iota(jnp.int32, shape, 1)

    def plus(coefficient, x):
        return x + jnp.where(diagonal, coefficient, 0.0)

    matrix = plus(1.0, matrix)
    norm = jnp.sqrt(jnp.sum(jnp.sum(matrix * matrix, axis=0, keepdims=True), axis=1, keepdims=True))
    y_ref[...] = matrix * (1.0 / norm)

    identity = 1.0
    for pair in range(3):
        y = y_ref[...]
        t = y
        if pair:
            t = identity * y + symmetric3(split(z_ref[...]), split(y))
        ts = split(t)
        square = symmetric3(ts, ts)
        extra = 1.6875 * square - 2.4375 * t + symmetric3(split(square), split(0.0625 * square - 0.5625 * t))
        es = split(extra)
        if pair < 2:
            y_ref[...] = 2.25 * y + symmetric3(split(y), es)
        if pair:
            z = z_ref[...]
            extra = 2.25 * z + identity * extra + symmetric3(es, split(z))
        z_ref[...] = extra
        identity = 2.25 * identity

    root = plus(identity, z_ref[...]) * (1.0 / jnp.sqrt(norm))
    projected = jnp.sum(proj_ref[...], axis=1, keepdims=True)
    once = jnp.sum(root * projected, axis=0, keepdims=True)
    once = jnp.broadcast_to(once, (8, MEMBERS)).T[:, 0:1]
    shift = jnp.sum(root * once, axis=0, keepdims=True)
    weights = split(root + shift)

    lane = lax.broadcasted_iota(jnp.int32, (MEMBERS, LANES), 1)
    low = (lane & 7) < 4
    even = (lane & 8) == 0

    def result_of(q, _):
        lanes = pl.ds(pl.multiple_of(q * LANES, LANES), LANES)
        cells = [
            jnp.concatenate([near[:, lanes], far[:, lanes]], axis=1)
            for near, far in ((ah_in_ref, ah_ref), (al_in_ref, al_ref))
        ]
        result = dot3(weights, cells)
        near = result[:, :LANES] + mean_in_ref[pl.ds(q, 1)]
        far = result[:, LANES:] + mean_ref[pl.ds(q, 1)]
        left = jnp.where(low, far, near)
        right = jnp.where(low, near, far)
        upper = jnp.where(even, left, pltpu.roll(right, 8, 1))
        lower = jnp.where(even, pltpu.roll(left, LANES - 8, 1), right)
        for strip, values in ((2 * q, upper), (2 * q + 1, lower)):
            place = strip_column(strip)
            for b in range(4):
                part = values[b * LANES : (b + 1) * LANES].reshape(2, 64, LANES)
                out_ref[pl.ds(place * 8 + ((b + place) & 3) * 2, 2)] = part
        return 0

    lax.fori_loop(0, 8, result_of, 0, unroll=4)


def vmem(count):
    return [pl.BlockSpec(memory_space=pltpu.VMEM) for _ in range(count)]


def in_vmem(x):
    return pltpu.with_memory_space_constraint(x, pltpu.VMEM)


def call(kernel, outs, scratch, limit, flops, name, *operands, specs=None):
    return pl.pallas_call(
        kernel,
        out_shape=[pltpu.VMEM(*out) for out in outs],
        in_specs=specs or vmem(len(operands)),
        out_specs=vmem(len(outs)),
        scratch_shapes=scratch,
        compiler_params=pltpu.CompilerParams(vmem_limit_bytes=limit * 2**20),
        cost_estimate=pl.CostEstimate(flops=flops, transcendentals=0, bytes_accessed=2**20),
        name=name,
    )(*operands)


def columns(count):
    return (64, count * 8, LANES), jnp.float32


def body(ensemble, obs_cells, obs_values, obs_rinv, obs_count):
    regions, block = ensemble.shape[0], ensemble.shape[1]
    following = OWNER[1:] + OWNER[:1]
    after = list(zip(OWNER, following))
    before = list(zip(following, OWNER))

    def exchange(x):
        return lax.all_to_all(x, MESH, split_axis=0, concat_axis=0, tiled=True, axis_index_groups=[OWNER])

    unit = 10**9

    slots = lax.broadcasted_iota(jnp.int32, obs_cells.shape, 1)
    active = (slots < obs_count[:, None]).astype(jnp.float32)
    rinv = obs_rinv * active / (MEMBERS - 1.0)
    grids = pl.pallas_call(
        obs_kernel, out_shape=pltpu.VMEM((32, LANES), jnp.float32), in_specs=vmem(3), out_specs=vmem(1)[0],
        compiler_params=pltpu.CompilerParams(vmem_limit_bytes=4 * 2**20), name="observations",
    )(obs_cells, rinv, obs_values)
    grids = lax.ppermute(grids, MESH, list(enumerate(OWNER)))
    pieces_in = exchange(ensemble.reshape(regions, block, LANES))
    pieces_in, grids = lax.optimization_barrier((pieces_in, grids))
    f32, bf16 = jnp.float32, jnp.bfloat16
    tiles, first, last = call(
        tiles_kernel, [columns(16), columns(HALO), columns(HALO)],
        [pltpu.VMEM((regions, block, LANES), f32), pltpu.SemaphoreType.DMA((16,))],
        8, unit, "tiles", pieces_in, specs=[pl.BlockSpec(memory_space=pl.ANY)],
    )
    west = lax.ppermute(last, MESH, after)
    east = lax.ppermute(first, MESH, before)
    *levels, inner = call(
        inner_kernel, [columns(14), columns(12), columns(10), columns(8)], [], 2, 4 * unit, "inner",
        in_vmem(tiles),
    )
    half = (MEMBERS, 1024), bf16
    square = (MEMBERS, MEMBERS), f32
    sums = (MEMBERS, LANES), f32
    means = (8, LANES), f32
    partial = call(
        inner_sums_kernel, [square, sums, means, half, half], [pltpu.VMEM(*half)] * 2,
        8, 6 * unit, "inner_sums", in_vmem(inner), in_vmem(grids),
    )
    inputs = [tiles, *levels, west, east, grids, *partial]
    (analysed,) = call(
        analysis_kernel,
        [((regions, block, LANES), f32)],
        [
            pltpu.VMEM(*shape)
            for shape in [columns(HALO)] * 6 + [columns(8), means] + [half] * 4 + [sums, square, square]
        ],
        24, 30 * unit, "analysis", *[in_vmem(x) for x in inputs],
    )
    return exchange(analysed).reshape(ensemble.shape)


def solution(mesh):
    return jax.shard_map(
        body,
        mesh=mesh,
        in_specs=(
            P(None, "mem", "space", None),
            P(("mem", "space"), None),
            P(("mem", "space"), None),
            P(("mem", "space"), None),
            P(("mem", "space")),
        ),
        out_specs=P(None, "mem", "space", None),
        check_vma=False,
    )
```
